32 devices in a mesh: tm: 8 (over z, y), space: 4 (over x, core).
Axes of the slice: x: 2, y: 2, z: 4, core: 2. Of those that a mesh axis runs over, the one named last changes fastest.
Arguments:
- starts: float32 [8, 5, 16, 64, 128], P('tm', None, 'space'), may hold values from -4 to 4
- source: float32 [5, 16, 64, 128], P(None, 'space'), may hold values from -4 to 4
Outputs:
- ends: float32 [8, 5, 16, 64, 128], P('tm', None, 'space')
- slice_norms: float32 [8], P('tm')
- total_norm: float32 [1], replicated
The draws below stay inside these ranges and needn't reach their ends.
All inputs are finite; a program needn't handle non-finite values.
Results may differ from the reference program's by a relative error of at most 0.0003.
Values sent between devices are 32-bit elements; how exact they have to be, the bound alone decides.
No kernel may reach another device: no remote copies, remote signals or barrier semaphores. Data moves between devices by JAX's collectives and lax.ppermute only.
A program may use at most 64 MiB of HBM per device.

```python
import math
import jax
import jax.numpy as jnp
from jax import lax

FIELDS = 5
NX = 128
NY = 64
STEPS = 1
NZ = 16
SLICES = 8


def block_levels(rng, dims, cuts, least, top_value):
    gain, own = 1.0, jax.random.fold_in(rng, 6)
    for position, parts in cuts:
        draws = jnp.exp(jax.random.uniform(jax.random.fold_in(own, position), (parts,), jnp.float32, least / len(cuts), top_value / len(cuts)))
        gain = gain * jnp.repeat(draws, dims[position] // parts).reshape([-1 if axis == position else 1 for axis in range(len(dims))])
    return gain


def normal_values(stream_key, extent, deviation, reach, split=(), kind=jnp.bfloat16):
    entries = jax.random.normal(stream_key, extent, jnp.float32) * deviation
    if len(split) > 0:
        entries = block_levels(stream_key, extent, split, -0.22, 0.18) * entries
    return jnp.clip(entries, min=-reach, max=reach).astype(kind)


def setup_inputs(seed: int = 0) -> dict:
    key_of = jax.random.split(jax.random.key(seed), 3)
    return {
        "starts": normal_values(key_of[0], (SLICES, FIELDS, NZ, NY, NX), 0.3, 4.0, ((0, 8), (2, 4)), jnp.float32),
        "source": normal_values(key_of[1], (FIELDS, NZ, NY, NX), 0.3, 4.0, ((1, 4),), jnp.float32),
    }


viscosity = 0.08
diffusivity = 0.05
compress_rate = 0.25
time_step = 0.5
diffusion_number = 0.08
advect_xaxis = 0.2
advect_yaxis = 0.15
advect_zaxis = 0.1
epsilon = 1e-06

def central(values, axis):
    return 0.5 * (jnp.roll(values, -1, axis) - jnp.roll(values, 1, axis))

def laplace(values):
    summed = -6.0 * values
    for axis in (0, 1, 2):
        summed = summed + jnp.roll(values, -1, axis) + jnp.roll(values, 1, axis)
    return summed

def tendency(state_now, source):
    speed_xaxis = advect_xaxis + state_now[0]
    speed_yaxis = advect_yaxis + state_now[1]
    speed_zaxis = advect_zaxis + state_now[2]

    def transport(quantity):
        return central(speed_xaxis * quantity, 2) + central(speed_yaxis * quantity, 1) + central(speed_zaxis * quantity, 0)
    pressure = state_now[3]
    xmomentum = -transport(state_now[0]) - central(pressure, 2) + viscosity * laplace(state_now[0])
    ymomentum = -transport(state_now[1]) - central(pressure, 1) + viscosity * laplace(state_now[1])
    zmomentum = -transport(state_now[2]) - central(pressure, 0) + viscosity * laplace(state_now[2])
    pressure_rate = -compress_rate * (central(state_now[0], 2) + central(state_now[1], 1) + central(state_now[2], 0))
    scalar_rate = -transport(state_now[4]) + diffusivity * laplace(state_now[4])
    return jnp.stack([xmomentum, ymomentum, zmomentum, pressure_rate, scalar_rate]) + source

def fine_run(current, source):
    for repeat in range(STEPS):
        section_one = tendency(current, source)
        section_two = tendency(current + 0.5 * time_step * section_one, source)
        section_three = tendency(current + 0.5 * time_step * section_two, source)
        section_four = tendency(current + time_step * section_three, source)
        current = current + time_step / 6.0 * (section_one + 2.0 * section_two + 2.0 * section_three + section_four)
    return current

def signed_angle(length):
    cell_ids = jnp.arange(length, dtype=jnp.int32)
    signed = (cell_ids + length // 2) % length - length // 2
    return (signed, 2.0 * math.pi / length * signed.astype(jnp.float32))

def coarse_symbol():
    zsigned, zangles = signed_angle(NZ)
    ysigned, yangles = signed_angle(NY)
    xsigned, xangles = signed_angle(NX)
    keeper = ((jnp.abs(ysigned) < NY // 8)[:, None] & (jnp.abs(xsigned) < NX // 16)[None, :]).astype(jnp.float32)
    real_part = 1.0 + diffusion_number * ((2.0 * jnp.cos(zangles) - 2.0)[:, None, None] + (2.0 * jnp.cos(yangles) - 2.0)[None, :, None] + (2.0 * jnp.cos(xangles) - 2.0)[None, None, :])
    imag_part = -(advect_zaxis * jnp.sin(zangles)[:, None, None] + advect_yaxis * jnp.sin(yangles)[None, :, None] + advect_xaxis * jnp.sin(xangles)[None, None, :])
    return lax.complex(real_part * keeper[None], imag_part * keeper[None])

def coarse(values, symbol):
    spectrum = jnp.fft.fftn(values, axes=(1, 2, 3))
    return jnp.real(jnp.fft.ifftn(spectrum * symbol, axes=(1, 2, 3)))

def reference(starts, source):

    def run_slice(begin_state):
        return fine_run(begin_state, source)
    fine = lax.map(run_slice, starts)
    symbol = coarse_symbol()

    def advance(carried, inputs_pair):
        old_start, fine_end = inputs_pair
        end_state = fine_end + coarse(carried - old_start, symbol)
        jump_size = end_state - fine_end
        return (end_state, (end_state, jnp.sum(jump_size * jump_size)))
    unused, (ends, sums) = lax.scan(advance, starts[0], (starts, fine))
    cell_total = FIELDS * NZ * NY * NX
    slice_norms = jnp.sqrt(sums / cell_total + epsilon)
    total_norm = jnp.sqrt(jnp.sum(sums) / (cell_total * SLICES) + epsilon).reshape(1)
    return (ends, slice_norms, total_norm)
```

```python
import functools
import math

import jax
import jax.numpy as jnp
import numpy as np
from jax import lax
from jax.experimental import pallas as pl
from jax.experimental.pallas import tpu as pltpu
from jax.sharding import PartitionSpec as P

viscosity = 0.08
diffusivity = 0.05
compress_rate = 0.25
time_step = 0.5
diffusion_number = 0.08
advect_xaxis = 0.2
advect_yaxis = 0.15
advect_zaxis = 0.1
epsilon = 1e-06
spread = (viscosity, viscosity, viscosity, None, diffusivity)


def hi_lo(table):
    table = np.asarray(table, np.float32)
    high = table.astype(jnp.bfloat16)
    low = (table - high.astype(np.float32)).astype(jnp.bfloat16)
    return high, low


@functools.lru_cache(None)
def make_tables(slab, width, rows, cols):
    depth = slab * width
    keep_y, keep_x = rows // 8, cols // 16
    ky = np.arange(2 * keep_y)
    ky = np.where(ky < keep_y, ky, ky - 2 * keep_y)
    kx = np.arange(keep_x)
    half = slab * 2 * keep_y
    turn = 2.0 * np.pi
    tables = {}
    angle = turn * kx[:, None] * np.arange(cols)[None, :] / cols
    wave = np.concatenate([np.cos(angle), -np.sin(angle)])
    high, low = hi_lo(wave)
    tables["xforward"] = np.block([[high, high], [low, np.zeros_like(low)]])
    weight = np.where(kx == 0, 1.0, 2.0)[:, None] / (depth * rows * cols)
    wave = np.concatenate([weight * np.cos(angle), -weight * np.sin(angle)])
    high, low = hi_lo(wave)
    tables["xinverse"] = np.concatenate([high, high, low])
    kz = np.arange(depth).reshape(width, 1, slab, 1)
    kyb = ky.reshape(1, 1, 1, -1)

    def joint(layers):
        layers = np.asarray(layers).reshape(-1, 1, 1, 1, 1, 1)
        cells = np.arange(rows).reshape(1, -1, 1, 1, 1, 1)
        theta = turn * (kz[None, None] * layers / depth + kyb[None, None] * cells / rows)
        return theta.reshape(-1, width, 1, slab, 2 * keep_y)

    def forward(layers):
        theta = joint(layers)
        c, s = np.cos(theta), np.sin(theta)
        real = np.concatenate([c, -s], axis=2)
        imag = np.concatenate([s, c], axis=2)
        count = theta.shape[0]
        return real.reshape(count, -1), imag.reshape(count, -1)

    inner = forward(range(slab))
    outer = forward([-1, slab])
    tables["yzforward"] = hi_lo(np.concatenate([inner[0], inner[1], outer[0], outer[1]]))
    theta = joint(range(slab))
    count = theta.shape[0]
    c, s = np.cos(theta), np.sin(theta)
    real = np.concatenate([c, -s], axis=2).reshape(count, -1).T
    imag = np.concatenate([s, c], axis=2).reshape(count, -1).T
    tables["yzinverse"] = hi_lo(np.concatenate([real, imag], axis=1))
    place = np.arange(width).reshape(-1, 1, 1, 1)
    theta = turn * ((kz.reshape(1, width, slab, 1) * place) % width) / width
    theta = np.broadcast_to(theta, (width, width, slab, 2 * keep_y)).reshape(width, width, half)
    c, s = np.cos(theta), np.sin(theta)
    tables["phase"] = np.stack(
        [np.concatenate([c, c], -1), np.concatenate([s, -s], -1)], axis=1
    ).astype(np.float32)
    tz = turn * np.arange(depth).reshape(width, 1, slab, 1) / depth
    ty = turn * ky.reshape(1, 1, 1, -1) / rows
    tx = turn * kx.reshape(1, -1, 1, 1) / cols
    keeper = (np.abs(ky) < keep_y).reshape(1, 1, 1, -1)
    real = 1.0 + diffusion_number * (2 * np.cos(tz) + 2 * np.cos(ty) + 2 * np.cos(tx) - 6.0)
    imag = -(advect_zaxis * np.sin(tz) + advect_yaxis * np.sin(ty) + advect_xaxis * np.sin(tx))
    real = (real * keeper).reshape(width, keep_x, half)
    imag = (imag * keeper).reshape(width, keep_x, half)
    tables["symbol"] = np.stack(
        [np.concatenate([real, real], -1), np.concatenate([-imag, imag], -1)], axis=1
    ).astype(np.float32)
    tables["share"] = np.broadcast_to(
        np.where(kx == 0, 1.0, 2.0)[:, None] / (depth * rows * cols), (keep_x, 2 * half)
    ).astype(np.float32)
    return tables


on_chip = pl.BlockSpec(memory_space=pltpu.VMEM)
in_scalars = pl.BlockSpec(memory_space=pltpu.SMEM)


def local_call(kernel, out_shape, operands, scratch=(), places=None):
    specs = [in_scalars if operand.dtype == jnp.int32 else on_chip for operand in operands]
    for index, spec in (places or {}).items():
        specs[index] = spec
    return pl.pallas_call(
        kernel,
        out_shape=out_shape,
        in_specs=specs,
        out_specs=jax.tree.map(lambda _: on_chip, out_shape),
        scratch_shapes=list(scratch),
        compiler_params=pltpu.CompilerParams(vmem_limit_bytes=16 * 1024 * 1024),
    )(*operands)


def split(values):
    high = values.astype(jnp.bfloat16)
    low = (values - high.astype(jnp.float32)).astype(jnp.bfloat16)
    return high, low


def dot(left, right):
    return jnp.dot(left, right, preferred_element_type=jnp.float32)


def three_pass(values, high_table, low_table):
    count = values.shape[0]
    high, low = split(values)
    both = dot(jnp.concatenate([high, low]), high_table)
    return both[:count] + both[count:] + dot(high, low_table)


def along_x(cells, table):
    high, low = split(cells)
    both = lax.dot_general(
        table,
        jnp.concatenate([high, low], axis=1),
        (((1,), (1,)), ((), ())),
        preferred_element_type=jnp.float32,
    )
    count = table.shape[0] // 2
    return both[:count] + both[count:]


def by_field(waves, fields, keep):
    lanes = waves.shape[1] // fields
    real = [waves[:keep, f * lanes : (f + 1) * lanes] for f in range(fields)]
    imag = [waves[keep:, f * lanes : (f + 1) * lanes] for f in range(fields)]
    return jnp.concatenate(real), jnp.concatenate(imag)


def flux(state, sign):
    u, v, w, p, s = state
    c = (0.5 * sign) * (advect_zaxis + w)
    momentum = viscosity + c
    return [
        momentum * u,
        momentum * v,
        momentum * w + (0.5 * sign) * p,
        (0.5 * sign * compress_rate) * w,
        (diffusivity + c) * s,
    ]


def level_rate(state, source):
    u, v, w, p, s = state
    rates = list(source)
    rows, cols = u.shape
    for axis, length, speed, velocity, lead in (
        (1, cols, advect_xaxis + u, u, 0),
        (0, rows, advect_yaxis + v, v, 1),
    ):
        half = 0.5 * speed
        for index, field in enumerate(state):
            if index == 3:
                plus = (0.5 * compress_rate) * velocity
                minus = -plus
            else:
                plus = (spread[index] + half) * field
                minus = (spread[index] - half) * field
            if index == lead:
                plus = plus + 0.5 * p
                minus = minus - 0.5 * p
            rates[index] = (
                rates[index] + pltpu.roll(plus, 1, axis) + pltpu.roll(minus, length - 1, axis)
            )
    for index, field in enumerate(state):
        if index != 3:
            rates[index] = rates[index] - (6.0 * spread[index]) * field
    return rates


def slab_rates(states, sources, put):
    slab = len(states)
    for layer in range(slab):
        rates = level_rate(states[layer](), sources[layer]())
        if layer > 0:
            rates = [r + g for r, g in zip(rates, flux(states[layer - 1](), 1.0))]
        if layer < slab - 1:
            rates = [r + g for r, g in zip(rates, flux(states[layer + 1](), -1.0))]
        put(layer, rates)


def reader(ref, layer):
    return lambda: [ref[f, layer] for f in range(ref.shape[0])]


def readers(ref):
    return [reader(ref, layer) for layer in range(ref.shape[1])]


def first_flux_kernel(state_ref, up_ref, down_ref, top_ref, bottom_ref, sems):
    last = state_ref.shape[1] - 1
    top = pltpu.make_async_copy(state_ref.at[:, last], top_ref, sems.at[0])
    bottom = pltpu.make_async_copy(state_ref.at[:, 0], bottom_ref, sems.at[1])
    top.start()
    bottom.start()
    fields = state_ref.shape[0]
    top.wait()
    for f, value in enumerate(flux([top_ref[f] for f in range(fields)], 1.0)):
        up_ref[f] = value
    bottom.wait()
    for f, value in enumerate(flux([bottom_ref[f] for f in range(fields)], -1.0)):
        down_ref[f] = value


def first_rate_kernel(state_ref, source_ref, table_ref, rate_ref, waves_ref):
    fields, slab, rows, cols = state_ref.shape

    def put(layer, rates):
        for f in range(fields):
            rate_ref[f, layer] = rates[f]

    slab_rates(readers(state_ref), readers(source_ref), put)
    keep = table_ref.shape[0] // 4
    cells = state_ref[...].reshape(fields * slab * rows, cols)
    real, imag = by_field(along_x(cells, table_ref[...]), fields, keep)
    lanes = real.shape[1]
    waves_ref[:, :lanes] = real
    waves_ref[:, lanes:] = imag


def edge_kernel(state_ref, rate_ref, below_ref, above_ref, edge_ref, up_ref, down_ref, *, step):
    fields, slab = state_ref.shape[:2]
    last = slab - 1
    top = [
        state_ref[f, last] + step * (rate_ref[f, last] + above_ref[f]) for f in range(fields)
    ]
    for f, value in enumerate(flux(top, 1.0)):
        edge_ref[1, f] = top[f]
        up_ref[f] = value
    bottom = [state_ref[f, 0] + step * (rate_ref[f, 0] + below_ref[f]) for f in range(fields)]
    for f, value in enumerate(flux(bottom, -1.0)):
        edge_ref[0, f] = bottom[f]
        down_ref[f] = value


def fill_stage(state_ref, rate_ref, edge_ref, stage_ref, step):
    fields, slab = state_ref.shape[:2]
    for f in range(fields):
        stage_ref[f, 0] = edge_ref[0, f]
        for layer in range(1, slab - 1):
            stage_ref[f, layer] = state_ref[f, layer] + step * rate_ref[f, layer]
        stage_ref[f, slab - 1] = edge_ref[1, f]


def rate_kernel(
    state_ref, rate_ref, edge_ref, source_ref, sum_ref, next_ref, total_ref, stage_ref, *, step, share
):
    fields = state_ref.shape[0]
    fill_stage(state_ref, rate_ref, edge_ref, stage_ref, step)

    def put(layer, rates):
        for f in range(fields):
            next_ref[f, layer] = rates[f]
            total_ref[f, layer] = sum_ref[f, layer] * share[0] + stage_ref[f, layer] * share[1]

    slab_rates(readers(stage_ref), readers(source_ref), put)


def forward_kernel(
    place_ref,
    state_ref,
    rate_ref,
    below_ref,
    above_ref,
    source_ref,
    sum_ref,
    shifted_ref,
    table_ref,
    high_ref,
    low_ref,
    phase_ref,
    out_ref,
    inner_ref,
    outer_ref,
    edge_ref,
    stage_ref,
    *,
    step,
    weight,
):
    fields, slab, rows, cols = state_ref.shape
    last = slab - 1
    for f in range(fields):
        edge_ref[0, f] = state_ref[f, 0] + step * (rate_ref[f, 0] + below_ref[f])
        edge_ref[1, f] = state_ref[f, last] + step * (rate_ref[f, last] + above_ref[f])
    fill_stage(state_ref, rate_ref, edge_ref, stage_ref, step)

    def put(layer, rates):
        for f in range(fields):
            inner_ref[f, layer] = (
                sum_ref[f, layer] + stage_ref[f, layer] * (1.0 / 3.0) + weight * rates[f]
            )

    slab_rates(readers(stage_ref), readers(source_ref), put)
    for f, value in enumerate(flux([edge_ref[0, f] for f in range(fields)], -1.0)):
        outer_ref[0, f] = weight * value
    for f, value in enumerate(flux([edge_ref[1, f] for f in range(fields)], 1.0)):
        outer_ref[1, f] = weight * value

    width = out_ref.shape[0]
    keep = table_ref.shape[0] // 4
    half = out_ref.shape[2] // 2
    place = place_ref[0]
    table = table_ref[...]
    real, imag = by_field(
        along_x(inner_ref[...].reshape(fields * slab * rows, cols), table), fields, keep
    )
    outer_cells = jnp.concatenate(
        [outer_ref[side, f] for f in range(fields) for side in range(2)]
    )
    outer_real, outer_imag = by_field(along_x(outer_cells, table), fields, keep)
    shifted = shifted_ref[...]
    lanes = real.shape[1]
    left = jnp.concatenate(
        [real - shifted[:, :lanes], imag - shifted[:, lanes:], outer_real, outer_imag], axis=1
    )
    waves = three_pass(left, high_ref[...], low_ref[...])
    for group in range(width):
        block = waves[:, group * 2 * half : (group + 1) * 2 * half]
        turned = (
            block * phase_ref[place, 0, group, :][None, :]
            + pltpu.roll(block, half, 1) * phase_ref[place, 1, group, :][None, :]
        )
        out_ref[lax.rem(group - place + width, width)] = turned


def coarse_kernel(place_ref, slot_ref, jump_ref, symbol_ref, share_ref, out_ref, kept_ref):
    slices, lines, lanes = jump_ref.shape
    keep = share_ref.shape[0]
    fields = lines // keep
    place = place_ref[0]
    moment = place_ref[1]
    real = symbol_ref[place, 0]
    imag = symbol_ref[place, 1]
    share = share_ref[...]
    current = [jnp.zeros((keep, lanes), jnp.float32) for _ in range(fields)]
    sizes = []
    kept_ref[0] = jnp.zeros((lines, lanes), jnp.float32)
    for moment_id in range(slices):
        total = jnp.zeros((keep, lanes), jnp.float32)
        for f in range(fields):
            total = total + current[f] * current[f]
        sizes.append(jnp.sum(total * share, axis=0, keepdims=True))
        if moment_id == slices - 1:
            break
        slot = slot_ref[moment_id]
        for f in range(fields):
            value = jump_ref[slot, f * keep : (f + 1) * keep, :] + current[f]
            current[f] = value * real + pltpu.roll(value, lanes // 2, 1) * imag
            kept_ref[moment_id + 1, f * keep : (f + 1) * keep, :] = current[f]
    out_ref[:lines, :] = kept_ref[moment]
    sums = jnp.sum(jnp.concatenate(sizes), axis=1, keepdims=True)
    spare = out_ref.shape[0] - lines - slices
    if spare > 0:
        out_ref[lines + slices :, :] = jnp.zeros((spare, lanes), jnp.float32)
    out_ref[lines : lines + slices, :] = jnp.broadcast_to(sums, (slices, lanes))


def inverse_kernel(
    place_ref,
    *refs,
    width,
    scales,
):
    block_refs = refs[:width]
    (
        fine_ref,
        below_ref,
        above_ref,
        high_ref,
        low_ref,
        table_ref,
        phase_ref,
        ends_ref,
        norm_ref,
        order_ref,
    ) = refs[width:]
    fields, slab, rows, cols = fine_ref.shape
    place = place_ref[0]
    moment = place_ref[1]
    lines, lanes = order_ref.shape[1:]
    keep = lines // fields
    sums = None
    for step in range(width):
        group = lax.rem(place - step + width, width)
        block = block_refs[step][:lines, :]
        order_ref[group] = (
            block * phase_ref[place, 0, group, :][None, :]
            - pltpu.roll(block, lanes // 2, 1) * phase_ref[place, 1, group, :][None, :]
        )
        part = block_refs[step][lines:, :]
        sums = part if sums is None else sums + part
    line = lax.broadcasted_iota(jnp.int32, sums.shape, 0)
    own = jnp.sum(jnp.where(line == moment, sums, 0.0), axis=0, keepdims=True)
    whole = jnp.sum(sums, axis=0, keepdims=True)
    norm_ref[0:1, :] = jnp.sqrt(own * scales[0] + epsilon)
    norm_ref[1:2, :] = jnp.sqrt(whole * scales[1] + epsilon)
    left = jnp.concatenate([order_ref[group] for group in range(width)], axis=1)
    waves = three_pass(left, high_ref[...], low_ref[...])
    count = slab * rows
    for f in range(fields):
        both = jnp.concatenate(
            [waves[f * keep : (f + 1) * keep, :count], waves[f * keep : (f + 1) * keep, count:]]
        )
        high, low = split(both)
        change = lax.dot_general(
            jnp.concatenate([high, low, high]),
            table_ref[...],
            (((0,), (0,)), ((), ())),
            preferred_element_type=jnp.float32,
        ).reshape(slab, rows, cols)
        for layer in range(slab):
            value = fine_ref[f, layer] + change[layer]
            if layer == 0:
                value = value + below_ref[f]
            if layer == slab - 1:
                value = value + above_ref[f]
            ends_ref[f, layer] = value


def halo(up, down):
    count = lax.axis_size("space")
    ups = [(i, (i + 1) % count) for i in range(count)]
    downs = [((i + 1) % count, i) for i in range(count)]
    return lax.ppermute(up, "space", ups), lax.ppermute(down, "space", downs)


def radices(count):
    parts = []
    while count % 4 == 0 and count > 4:
        parts.append(4)
        count //= 4
    if count > 1:
        parts.append(count)
    return sorted(parts)


def shards(starts, source):
    state_now = starts[0]
    fields, slab, rows, cols = state_now.shape
    width = lax.axis_size("space")
    slices = lax.axis_size("tm")
    depth = slab * width
    keep_y, keep_x = rows // 8, cols // 16
    lines, lanes = fields * keep_x, 2 * slab * 2 * keep_y
    tables = make_tables(slab, width, rows, cols)
    place = lax.axis_index("space").astype(jnp.int32)
    moment = lax.axis_index("tm").astype(jnp.int32)
    where = jnp.stack([place, moment])
    real = jnp.float32

    layer_shape = jax.ShapeDtypeStruct((fields, rows, cols), real)
    edge_shape = jax.ShapeDtypeStruct((2, fields, rows, cols), real)
    slab_shape = jax.ShapeDtypeStruct((fields, slab, rows, cols), real)
    layer = pltpu.VMEM((fields, rows, cols), real)
    whole_slab = pltpu.VMEM((fields, slab, rows, cols), real)

    up, down = local_call(
        first_flux_kernel,
        (layer_shape, layer_shape),
        [state_now],
        [layer, layer, pltpu.SemaphoreType.DMA((2,))],
        {0: pl.BlockSpec(memory_space=pl.ANY)},
    )
    below, above = halo(up, down)
    rates, start_waves = local_call(
        first_rate_kernel,
        (slab_shape, jax.ShapeDtypeStruct((lines, 2 * slab * rows), real)),
        [state_now, source, tables["xforward"]],
    )
    next_waves = lax.ppermute(start_waves, "tm", [(i + 1, i) for i in range(slices - 1)])
    total = state_now
    for stage in range(2):
        step = 0.5 * time_step
        edge, up, down = local_call(
            functools.partial(edge_kernel, step=step),
            (edge_shape, layer_shape, layer_shape),
            [state_now, rates, below, above],
        )
        below, above = halo(up, down)
        share = ((-1.0 / 3.0, 1.0 / 3.0), (1.0, 2.0 / 3.0))[stage]
        rates, total = local_call(
            functools.partial(rate_kernel, step=step, share=share),
            (slab_shape, slab_shape),
            [state_now, rates, edge, source, total],
            [whole_slab],
        )
    waves, fine_inner, fine_outer = local_call(
        functools.partial(forward_kernel, step=time_step, weight=time_step / 6.0),
        (
            jax.ShapeDtypeStruct((width, lines, lanes), real),
            slab_shape,
            edge_shape,
        ),
        [
            where,
            state_now,
            rates,
            below,
            above,
            source,
            total,
            next_waves,
            tables["xforward"],
            *tables["yzforward"],
            tables["phase"],
        ],
        [pltpu.VMEM((2, fields, rows, cols), real), whole_slab],
    )
    jump = waves[0]
    for step in range(1, width):
        jump = jump + lax.ppermute(
            waves[step], "space", [(i, (i + step) % width) for i in range(width)]
        )

    up, down, jump = lax.optimization_barrier((fine_outer[1], fine_outer[0], jump))
    below, above = halo(up, down)

    jumps = jump[None]
    stride = 1
    slots = jnp.zeros((slices,), jnp.int32)
    ids = jnp.arange(slices, dtype=jnp.int32)
    for radix in radices(slices):
        parts = [jumps]
        for step in range(1, radix):
            pairs = []
            for i in range(slices):
                digit = i // stride % radix
                pairs.append((i, i + ((digit + step) % radix - digit) * stride))
            parts.append(lax.ppermute(jumps, "tm", pairs))
        jumps = jnp.concatenate(parts)
        slots = slots + (moment // stride - ids // stride) % radix * stride
        stride *= radix

    message = local_call(
        coarse_kernel,
        jax.ShapeDtypeStruct((lines + -(-slices // 8) * 8, lanes), real),
        [where, slots, jumps, tables["symbol"], tables["share"]],
        [pltpu.VMEM((slices, lines, lanes), real)],
    )
    blocks = [message]
    for step in range(1, width):
        blocks.append(
            lax.ppermute(message, "space", [(i, (i + step) % width) for i in range(width)])
        )
    cells = fields * depth * rows * cols
    ends, norms = local_call(
        functools.partial(
            inverse_kernel, width=width, scales=(1.0 / cells, 1.0 / (cells * slices))
        ),
        (
            jax.ShapeDtypeStruct((fields, slab, rows, cols), real),
            jax.ShapeDtypeStruct((2, lanes), real),
        ),
        [
            where,
            *blocks,
            fine_inner,
            below,
            above,
            *tables["yzinverse"],
            tables["xinverse"],
            tables["phase"],
        ],
        [pltpu.VMEM((width, lines, lanes), real)],
    )
    return ends[None], norms[0, :1], norms[1, :1]


def solution(mesh):
    in_specs = (P("tm", None, "space", None, None), P(None, "space", None, None))
    out_specs = (P("tm", None, "space", None, None), P("tm"), P())
    return jax.shard_map(shards, mesh=mesh, in_specs=in_specs, out_specs=out_specs, check_vma=False)
```

```python
import functools

import jax
import jax.numpy as jnp
import numpy as np
from jax import lax
from jax.experimental import pallas as pl
from jax.experimental.pallas import tpu as pltpu
from jax.sharding import PartitionSpec as P


viscosity = 0.08
diffusivity = 0.05
compress_rate = 0.25
time_step = 0.5
diffusion_number = 0.08
advect_xaxis = 0.2
advect_yaxis = 0.15
advect_zaxis = 0.1
epsilon = 1e-06
spread = (viscosity, viscosity, viscosity, None, diffusivity)


def hi_lo(table):
    table = np.asarray(table, np.float32)
    high = table.astype(jnp.bfloat16)
    low = (table - high.astype(np.float32)).astype(jnp.bfloat16)
    return high, low


@functools.lru_cache(None)
def make_tables(slab, width, rows, cols):
    depth = slab * width
    keep_y, keep_x = rows // 8, cols // 16
    ky = np.arange(2 * keep_y)
    ky = np.where(ky < keep_y, ky, ky - 2 * keep_y)
    kx = np.arange(keep_x)
    half = slab * 2 * keep_y
    turn = 2.0 * np.pi
    tables = {}
    angle = turn * kx[:, None] * np.arange(cols)[None, :] / cols
    wave = np.concatenate([np.cos(angle), -np.sin(angle)])
    high, low = hi_lo(wave)
    tables["xforward"] = np.block([[high, high], [low, np.zeros_like(low)]])
    weight = np.where(kx == 0, 1.0, 2.0)[:, None] / (depth * rows * cols)
    wave = np.concatenate([weight * np.cos(angle), -weight * np.sin(angle)])
    high, low = hi_lo(wave)
    tables["xinverse"] = np.concatenate([high, high, low])
    kz = np.arange(depth).reshape(width, 1, slab, 1)
    kyb = ky.reshape(1, 1, 1, -1)

    def joint(layers):
        layers = np.asarray(layers).reshape(-1, 1, 1, 1, 1, 1)
        cells = np.arange(rows).reshape(1, -1, 1, 1, 1, 1)
        theta = turn * (kz[None, None] * layers / depth + kyb[None, None] * cells / rows)
        return theta.reshape(-1, width, 1, slab, 2 * keep_y)

    def forward(layers):
        theta = joint(layers)
        c, s = np.cos(theta), np.sin(theta)
        real = np.concatenate([c, -s], axis=2)
        imag = np.concatenate([s, c], axis=2)
        count = theta.shape[0]
        return real.reshape(count, -1), imag.reshape(count, -1)

    inner = forward(range(slab))
    outer = forward([-1, slab])
    tables["yzforward"] = hi_lo(np.concatenate([inner[0], inner[1], outer[0], outer[1]]))
    theta = joint(range(slab))
    count = theta.shape[0]
    c, s = np.cos(theta), np.sin(theta)
    real = np.concatenate([c, -s], axis=2).reshape(count, -1).T
    imag = np.concatenate([s, c], axis=2).reshape(count, -1).T
    tables["yzinverse"] = hi_lo(np.concatenate([real, imag], axis=1))
    place = np.arange(width).reshape(-1, 1, 1, 1)
    theta = turn * ((kz.reshape(1, width, slab, 1) * place) % width) / width
    theta = np.broadcast_to(theta, (width, width, slab, 2 * keep_y)).reshape(width, width, half)
    c, s = np.cos(theta), np.sin(theta)
    tables["phase"] = np.stack(
        [np.concatenate([c, c], -1), np.concatenate([s, -s], -1)], axis=1
    ).astype(np.float32)
    tz = turn * np.arange(depth).reshape(width, 1, slab, 1) / depth
    ty = turn * ky.reshape(1, 1, 1, -1) / rows
    tx = turn * kx.reshape(1, -1, 1, 1) / cols
    keeper = (np.abs(ky) < keep_y).reshape(1, 1, 1, -1)
    real = 1.0 + diffusion_number * (2 * np.cos(tz) + 2 * np.cos(ty) + 2 * np.cos(tx) - 6.0)
    imag = -(advect_zaxis * np.sin(tz) + advect_yaxis * np.sin(ty) + advect_xaxis * np.sin(tx))
    real = (real * keeper).reshape(width, keep_x, half)
    imag = (imag * keeper).reshape(width, keep_x, half)
    tables["symbol"] = np.stack(
        [np.concatenate([real, real], -1), np.concatenate([-imag, imag], -1)], axis=1
    ).astype(np.float32)
    tables["share"] = np.broadcast_to(
        np.where(kx == 0, 1.0, 2.0)[:, None] / (depth * rows * cols), (keep_x, 2 * half)
    ).astype(np.float32)
    return tables


on_chip = pl.BlockSpec(memory_space=pltpu.VMEM)
off_chip = pl.BlockSpec(memory_space=pltpu.HBM)
in_scalars = pl.BlockSpec(memory_space=pltpu.SMEM)


def local_call(kernel, out_shape, operands, scratch=(), places=None, out_specs=None):
    specs = [in_scalars if operand.dtype == jnp.int32 else on_chip for operand in operands]
    for index, spec in (places or {}).items():
        specs[index] = spec
    if out_specs is None:
        out_specs = jax.tree.map(lambda _: on_chip, out_shape)
        out_shape = jax.tree.map(lambda out: pltpu.VMEM(out.shape, out.dtype), out_shape)
    return pl.pallas_call(
        kernel,
        out_shape=out_shape,
        in_specs=specs,
        out_specs=out_specs,
        scratch_shapes=list(scratch),
        compiler_params=pltpu.CompilerParams(vmem_limit_bytes=16 * 1024 * 1024),
    )(*operands)


def split(values):
    high = values.astype(jnp.bfloat16)
    low = (values - high.astype(jnp.float32)).astype(jnp.bfloat16)
    return high, low


def dot(left, right):
    return jnp.dot(left, right, preferred_element_type=jnp.float32)


def three_pass(values, high_table, low_table):
    count = values.shape[0]
    high, low = split(values)
    both = dot(jnp.concatenate([high, low]), high_table)
    return both[:count] + both[count:] + dot(high, low_table)


def along_x(cells, table):
    high, low = split(cells)
    both = lax.dot_general(
        table,
        jnp.concatenate([high, low], axis=1),
        (((1,), (1,)), ((), ())),
        preferred_element_type=jnp.float32,
    )
    count = table.shape[0] // 2
    return both[:count] + both[count:]


def by_field(waves, fields, keep):
    lanes = waves.shape[1] // fields
    real = [waves[:keep, f * lanes : (f + 1) * lanes] for f in range(fields)]
    imag = [waves[keep:, f * lanes : (f + 1) * lanes] for f in range(fields)]
    return jnp.concatenate(real), jnp.concatenate(imag)


def flux(state, sign):
    u, v, w, p, s = state
    c = (0.5 * sign) * (advect_zaxis + w)
    momentum = viscosity + c
    return [
        momentum * u,
        momentum * v,
        momentum * w + (0.5 * sign) * p,
        (0.5 * sign * compress_rate) * w,
        (diffusivity + c) * s,
    ]


def level_rate(state, source):
    u, v, _, p, _ = state
    rates = list(source)
    rows, cols = u.shape
    for axis, length, speed, velocity, lead in (
        (1, cols, advect_xaxis + u, u, 0),
        (0, rows, advect_yaxis + v, v, 1),
    ):
        half = 0.5 * speed
        for index, field in enumerate(state):
            if index == 3:
                plus = (0.5 * compress_rate) * velocity
                minus = -plus
            else:
                plus = (spread[index] + half) * field
                minus = (spread[index] - half) * field
            if index == lead:
                plus = plus + 0.5 * p
                minus = minus - 0.5 * p
            rates[index] = (
                rates[index] + pltpu.roll(plus, 1, axis) + pltpu.roll(minus, length - 1, axis)
            )
    for index, field in enumerate(state):
        if index != 3:
            rates[index] = rates[index] - (6.0 * spread[index]) * field
    return rates


def slab_rates(states, sources, put):
    slab = len(states)
    for layer in range(slab):
        rates = level_rate(states[layer](), sources[layer]())
        if layer > 0:
            rates = [r + g for r, g in zip(rates, flux(states[layer - 1](), 1.0))]
        if layer < slab - 1:
            rates = [r + g for r, g in zip(rates, flux(states[layer + 1](), -1.0))]
        put(layer, rates)


def reader(ref, layer):
    return lambda: [ref[f, layer] for f in range(ref.shape[0])]


def readers(ref):
    return [reader(ref, layer) for layer in range(ref.shape[1])]


def first_flux_kernel(state_ref, *out_refs):
    parts = len(out_refs) // 2
    fields, slab, rows, _ = state_ref.shape
    count = rows // parts
    for part in range(parts):
        span = pl.ds(part * count, count)
        for side, (layer, sign) in enumerate(((slab - 1, 1.0), (0, -1.0))):
            values = [state_ref[f, layer, span] for f in range(fields)]
            for f, value in enumerate(flux(values, sign)):
                out_refs[2 * part + side][f] = value


def first_rate_kernel(state_ref, source_ref, table_ref, rate_ref, waves_ref):
    fields, slab, rows, cols = state_ref.shape

    def put(layer, rates):
        for f in range(fields):
            rate_ref[f, layer] = rates[f]

    slab_rates(readers(state_ref), readers(source_ref), put)
    keep = table_ref.shape[0] // 4
    cells = state_ref[...].reshape(fields * slab * rows, cols)
    real, imag = by_field(along_x(cells, table_ref[...]), fields, keep)
    lanes = real.shape[1]
    waves_ref[:, :lanes] = real
    waves_ref[:, lanes:] = imag


def edge_kernel(
    state_ref, rate_ref, below_ref, above_ref, edge_ref, up_ref, down_ref, *, step, part
):
    fields, slab = state_ref.shape[:2]
    last = slab - 1
    count = below_ref.shape[1]
    span = pl.ds(part * count, count)
    for side, layer, came_ref, out_ref, sign in (
        (1, last, above_ref, up_ref, 1.0),
        (0, 0, below_ref, down_ref, -1.0),
    ):
        values = [
            state_ref[f, layer, span] + step * (rate_ref[f, layer, span] + came_ref[f])
            for f in range(fields)
        ]
        for f, value in enumerate(flux(values, sign)):
            edge_ref[side, f] = values[f]
            out_ref[f] = value


def fill_stage(state_ref, rate_ref, edge_refs, stage_ref, step):
    fields, slab = state_ref.shape[:2]
    for f in range(fields):
        for part, edge_ref in enumerate(edge_refs):
            count = edge_ref.shape[2]
            span = pl.ds(part * count, count)
            stage_ref[f, 0, span] = edge_ref[0, f]
            stage_ref[f, slab - 1, span] = edge_ref[1, f]
        for layer in range(1, slab - 1):
            stage_ref[f, layer] = state_ref[f, layer] + step * rate_ref[f, layer]


def rate_kernel(state_ref, rate_ref, source_ref, sum_ref, *refs, step, share):
    *edge_refs, next_ref, total_ref, stage_ref = refs
    fields = state_ref.shape[0]
    fill_stage(state_ref, rate_ref, edge_refs, stage_ref, step)

    def put(layer, rates):
        for f in range(fields):
            next_ref[f, layer] = rates[f]
            total_ref[f, layer] = sum_ref[f, layer] * share[0] + stage_ref[f, layer] * share[1]

    slab_rates(readers(stage_ref), readers(source_ref), put)


def forward_kernel(
    state_ref,
    rate_ref,
    source_ref,
    sum_ref,
    shifted_ref,
    table_ref,
    high_ref,
    low_ref,
    phase_ref,
    *refs,
    step,
    weight,
):
    *came_refs, out_ref, inner_ref, outer_ref, edge_ref, stage_ref = refs
    fields, slab, rows, cols = state_ref.shape
    last = slab - 1
    parts = len(came_refs) // 2
    count = rows // parts
    for part in range(parts):
        span = pl.ds(part * count, count)
        below_ref, above_ref = came_refs[2 * part : 2 * part + 2]
        for f in range(fields):
            edge_ref[0, f, span] = state_ref[f, 0, span] + step * (
                rate_ref[f, 0, span] + below_ref[f]
            )
            edge_ref[1, f, span] = state_ref[f, last, span] + step * (
                rate_ref[f, last, span] + above_ref[f]
            )
    fill_stage(state_ref, rate_ref, [edge_ref], stage_ref, step)

    def put(layer, rates):
        for f in range(fields):
            inner_ref[f, layer] = (
                sum_ref[f, layer] + stage_ref[f, layer] * (1.0 / 3.0) + weight * rates[f]
            )

    slab_rates(readers(stage_ref), readers(source_ref), put)
    for f, value in enumerate(flux([edge_ref[0, f] for f in range(fields)], -1.0)):
        outer_ref[0, f] = weight * value
    for f, value in enumerate(flux([edge_ref[1, f] for f in range(fields)], 1.0)):
        outer_ref[1, f] = weight * value

    width = out_ref.shape[0]
    keep = table_ref.shape[0] // 4
    half = out_ref.shape[2] // 2
    place = lax.axis_index("space")
    table = table_ref[...]
    real, imag = by_field(
        along_x(inner_ref[...].reshape(fields * slab * rows, cols), table), fields, keep
    )
    outer_cells = jnp.concatenate(
        [outer_ref[side, f] for f in range(fields) for side in range(2)]
    )
    outer_real, outer_imag = by_field(along_x(outer_cells, table), fields, keep)
    shifted = shifted_ref[...]
    lanes = real.shape[1]
    left = jnp.concatenate(
        [real - shifted[:, :lanes], imag - shifted[:, lanes:], outer_real, outer_imag], axis=1
    )
    waves = three_pass(left, high_ref[...], low_ref[...])
    for group in range(width):
        block = waves[:, group * 2 * half : (group + 1) * 2 * half]
        turned = (
            block * phase_ref[place, 0, group, :][None, :]
            + pltpu.roll(block, half, 1) * phase_ref[place, 1, group, :][None, :]
        )
        out_ref[lax.rem(group - place + width, width)] = turned


def slot_of(moment, moment_id, slices):
    slot, stride = 0, 1
    for radix in radices(slices):
        ours = lax.rem(moment // stride, radix)
        slot = slot + lax.rem(ours + (radix - moment_id // stride % radix), radix) * stride
        stride *= radix
    return slot


def coarse_kernel(jump_ref, symbol_ref, share_ref, out_ref, kept_ref):
    slices, lines, lanes = jump_ref.shape
    keep = share_ref.shape[0]
    fields = lines // keep
    place = lax.axis_index("space")
    moment = lax.axis_index("tm")
    real = symbol_ref[place, 0]
    imag = symbol_ref[place, 1]
    share = share_ref[...]
    blank = jnp.zeros((keep, lanes), jnp.float32)
    current = [(blank, blank)] * fields
    sizes = []
    kept_ref[0] = jnp.zeros((lines, lanes), jnp.float32)
    for moment_id in range(slices):
        total = blank
        for value, _ in current:
            total = total + value * value
        sizes.append(jnp.sum(total * share, axis=0, keepdims=True))
        if moment_id == slices - 1:
            break
        slot = slot_of(moment, moment_id, slices)
        for f in range(fields):
            jump = jump_ref[slot, f * keep : (f + 1) * keep, :]
            value = jump + current[f][0]
            swapped = pltpu.roll(jump, lanes // 2, 1) + current[f][1]
            current[f] = (value * real + swapped * imag, swapped * real - value * imag)
            kept_ref[moment_id + 1, f * keep : (f + 1) * keep, :] = current[f][0]
    out_ref[:lines, :] = kept_ref[moment]
    sums = jnp.sum(jnp.concatenate(sizes), axis=1, keepdims=True)
    spare = out_ref.shape[0] - lines - slices
    if spare > 0:
        out_ref[lines + slices :, :] = jnp.zeros((spare, lanes), jnp.float32)
    out_ref[lines : lines + slices, :] = jnp.broadcast_to(sums, (slices, lanes))


def inverse_kernel(*refs, width, scales):
    block_refs = refs[:width]
    (
        fine_ref,
        below_ref,
        above_ref,
        high_ref,
        low_ref,
        table_ref,
        phase_ref,
        ends_ref,
        slice_ref,
        total_ref,
        order_ref,
        held_ref,
        norm_refs,
        sems,
        norm_sems,
    ) = refs[width:]
    fields, slab, rows, cols = fine_ref.shape
    place = lax.axis_index("space")
    moment = lax.axis_index("tm")
    lines, lanes = order_ref.shape[1:]
    keep = lines // fields
    sums = None
    for step in range(width):
        group = lax.rem(place - step + width, width)
        block = block_refs[step][:lines, :]
        order_ref[group] = (
            block * phase_ref[place, 0, group, :][None, :]
            - pltpu.roll(block, lanes // 2, 1) * phase_ref[place, 1, group, :][None, :]
        )
        part = block_refs[step][lines:, :]
        sums = part if sums is None else sums + part
    left = jnp.concatenate([order_ref[group] for group in range(width)], axis=1)
    waves = three_pass(left, high_ref[...], low_ref[...])
    count = slab * rows
    copies = []
    for f in range(fields):
        both = jnp.concatenate(
            [waves[f * keep : (f + 1) * keep, :count], waves[f * keep : (f + 1) * keep, count:]]
        )
        high, low = split(both)
        change = lax.dot_general(
            jnp.concatenate([high, low, high]),
            table_ref[...],
            (((0,), (0,)), ((), ())),
            preferred_element_type=jnp.float32,
        ).reshape(slab, rows, cols)
        for layer in range(slab):
            value = fine_ref[f, layer] + change[layer]
            if layer == 0:
                value = value + below_ref[f]
            if layer == slab - 1:
                value = value + above_ref[f]
            held_ref[f, layer] = value
        copies.append(pltpu.make_async_copy(held_ref.at[f], ends_ref.at[f], sems.at[f]))
        copies[-1].start()
    line = lax.broadcasted_iota(jnp.int32, sums.shape, 0)
    own = jnp.sum(jnp.where(line == moment, sums, 0.0), axis=0, keepdims=True)
    whole = jnp.sum(sums, axis=0, keepdims=True)
    norm_refs[0, 0] = jnp.sqrt(own * scales[0] + epsilon)[0, 0]
    norm_refs[1, 0] = jnp.sqrt(whole * scales[1] + epsilon)[0, 0]
    for side, out_ref in enumerate((slice_ref, total_ref)):
        copies.append(pltpu.make_async_copy(norm_refs.at[side], out_ref, norm_sems.at[side]))
        copies[-1].start()
    for copy in copies:
        copy.wait()


def halo(up, down):
    count = lax.axis_size("space")
    ups = [(i, (i + 1) % count) for i in range(count)]
    downs = [((i + 1) % count, i) for i in range(count)]
    return lax.ppermute(up, "space", ups), lax.ppermute(down, "space", downs)


def radices(count):
    parts = []
    while count % 4 == 0 and count > 4:
        parts.append(4)
        count //= 4
    if count > 1:
        parts.append(count)
    return sorted(parts)


def shards(starts, source):
    state_now = starts[0]
    fields, slab, rows, cols = state_now.shape
    width = lax.axis_size("space")
    slices = lax.axis_size("tm")
    depth = slab * width
    keep_y, keep_x = rows // 8, cols // 16
    lines, lanes = fields * keep_x, 2 * slab * 2 * keep_y
    tables = make_tables(slab, width, rows, cols)
    real = jnp.float32

    parts = 2 if rows % 16 == 0 else 1
    layer_shape = jax.ShapeDtypeStruct((fields, rows // parts, cols), real)
    edge_shape = jax.ShapeDtypeStruct((2, fields, rows // parts, cols), real)
    slab_shape = jax.ShapeDtypeStruct((fields, slab, rows, cols), real)
    whole_slab = pltpu.VMEM((fields, slab, rows, cols), real)

    given = local_call(
        first_flux_kernel,
        (layer_shape,) * (2 * parts),
        [state_now],
    )
    came = [halo(*given[2 * part : 2 * part + 2]) for part in range(parts)]
    rates, start_waves = local_call(
        first_rate_kernel,
        (slab_shape, jax.ShapeDtypeStruct((lines, 2 * slab * rows), real)),
        [state_now, source, tables["xforward"]],
    )
    next_waves = lax.ppermute(start_waves, "tm", [(i + 1, i) for i in range(slices - 1)])
    total = state_now
    for stage in range(2):
        step = 0.5 * time_step
        edges, arrived = [], came
        came = []
        for part in range(parts):
            edge, up, down = local_call(
                functools.partial(edge_kernel, step=step, part=part),
                (edge_shape, layer_shape, layer_shape),
                [state_now, rates, *arrived[part]],
            )
            edges.append(edge)
            came.append(halo(up, down))
        share = ((-1.0 / 3.0, 1.0 / 3.0), (1.0, 2.0 / 3.0))[stage]
        rates, total = local_call(
            functools.partial(rate_kernel, step=step, share=share),
            (slab_shape, slab_shape),
            [state_now, rates, source, total, *edges],
            [whole_slab],
        )
    waves, fine_inner, fine_outer = local_call(
        functools.partial(forward_kernel, step=time_step, weight=time_step / 6.0),
        (
            jax.ShapeDtypeStruct((width, lines, lanes), real),
            slab_shape,
            jax.ShapeDtypeStruct((2, fields, rows, cols), real),
        ),
        [
            state_now,
            rates,
            source,
            total,
            next_waves,
            tables["xforward"],
            *tables["yzforward"],
            tables["phase"],
            *[array for pair in came for array in pair],
        ],
        [pltpu.VMEM((2, fields, rows, cols), real), whole_slab],
    )
    jump = waves[0]
    for step in range(1, width):
        part = lax.ppermute(waves[step], "space", [(i, (i + step) % width) for i in range(width)])
        jump = jump + part

    below, above = halo(fine_outer[1], fine_outer[0])

    jumps = jump[None]
    stride = 1
    for radix in radices(slices):
        parts = [jumps]
        for step in range(1, radix):
            pairs = []
            for i in range(slices):
                digit = i // stride % radix
                pairs.append((i, i + ((digit + step) % radix - digit) * stride))
            parts.append(lax.ppermute(jumps, "tm", pairs))
        jumps = jnp.concatenate(parts)
        stride *= radix

    message = local_call(
        coarse_kernel,
        jax.ShapeDtypeStruct((lines + -(-slices // 8) * 8, lanes), real),
        [jumps, tables["symbol"], tables["share"]],
        [pltpu.VMEM((slices, lines, lanes), real)],
    )
    blocks = [message]
    for step in range(1, width):
        blocks.append(
            lax.ppermute(message, "space", [(i, (i + step) % width) for i in range(width)])
        )
    cells = fields * depth * rows * cols
    ends, slice_norm, total_norm = local_call(
        functools.partial(
            inverse_kernel, width=width, scales=(1.0 / cells, 1.0 / (cells * slices))
        ),
        (
            jax.ShapeDtypeStruct((fields, slab, rows, cols), real),
            jax.ShapeDtypeStruct((1,), real),
            jax.ShapeDtypeStruct((1,), real),
        ),
        [
            *blocks,
            fine_inner,
            below,
            above,
            *tables["yzinverse"],
            tables["xinverse"],
            tables["phase"],
        ],
        [
            pltpu.VMEM((width, lines, lanes), real),
            whole_slab,
            pltpu.SMEM((2, 1), real),
            pltpu.SemaphoreType.DMA((fields,)),
            pltpu.SemaphoreType.DMA((2,)),
        ],
        out_specs=(off_chip, off_chip, off_chip),
    )
    return ends[None], slice_norm, total_norm


def solution(mesh):
    in_specs = (P("tm", None, "space", None, None), P(None, "space", None, None))
    out_specs = (P("tm", None, "space", None, None), P("tm"), P())
    return jax.shard_map(shards, mesh=mesh, in_specs=in_specs, out_specs=out_specs, check_vma=False)
```

```python
import functools

import jax
import jax.numpy as jnp
import numpy as np
from jax import lax
from jax.experimental import pallas as pl
from jax.experimental.pallas import tpu as pltpu
from jax.sharding import PartitionSpec as P


viscosity = 0.08
diffusivity = 0.05
compress_rate = 0.25
time_step = 0.5
diffusion_number = 0.08
advect_xaxis = 0.2
advect_yaxis = 0.15
advect_zaxis = 0.1
epsilon = 1e-06
spread = (viscosity, viscosity, viscosity, None, diffusivity)


def hi_lo(table):
    table = np.asarray(table, np.float32)
    high = table.astype(jnp.bfloat16)
    low = (table - high.astype(np.float32)).astype(jnp.bfloat16)
    return high, low


@functools.lru_cache(None)
def make_tables(slab, width, rows, cols):
    depth = slab * width
    keep_y, keep_x = rows // 8, cols // 16
    ky = np.arange(2 * keep_y)
    ky = np.where(ky < keep_y, ky, ky - 2 * keep_y)
    kx = np.arange(keep_x)
    half = slab * 2 * keep_y
    turn = 2.0 * np.pi
    tables = {}
    angle = turn * kx[:, None] * np.arange(cols)[None, :] / cols
    wave = np.concatenate([np.cos(angle), -np.sin(angle)])
    high, low = hi_lo(wave)
    tables["xforward"] = np.block([[high, high], [low, np.zeros_like(low)]])
    weight = np.where(kx == 0, 1.0, 2.0)[:, None] / (depth * rows * cols)
    wave = np.concatenate([weight * np.cos(angle), -weight * np.sin(angle)])
    high, low = hi_lo(wave)
    tables["xinverse"] = np.concatenate([high, high, low])
    kz = np.arange(depth).reshape(width, 1, slab, 1)
    kyb = ky.reshape(1, 1, 1, -1)

    def joint(layers):
        layers = np.asarray(layers).reshape(-1, 1, 1, 1, 1, 1)
        cells = np.arange(rows).reshape(1, -1, 1, 1, 1, 1)
        theta = turn * (kz[None, None] * layers / depth + kyb[None, None] * cells / rows)
        return theta.reshape(-1, width, 1, slab, 2 * keep_y)

    def forward(layers):
        theta = joint(layers)
        c, s = np.cos(theta), np.sin(theta)
        real = np.concatenate([c, -s], axis=2)
        imag = np.concatenate([s, c], axis=2)
        count = theta.shape[0]
        return real.reshape(count, -1), imag.reshape(count, -1)

    inner = forward(range(slab))
    outer = forward([-1, slab])
    tables["yzforward"] = hi_lo(np.concatenate([inner[0], inner[1], outer[0], outer[1]]))
    theta = joint(range(slab))
    count = theta.shape[0]
    c, s = np.cos(theta), np.sin(theta)
    real = np.concatenate([c, -s], axis=2).reshape(count, -1).T
    imag = np.concatenate([s, c], axis=2).reshape(count, -1).T
    tables["yzinverse"] = hi_lo(np.concatenate([real, imag], axis=1))
    place = np.arange(width).reshape(-1, 1, 1, 1)
    theta = turn * ((kz.reshape(1, width, slab, 1) * place) % width) / width
    theta = np.broadcast_to(theta, (width, width, slab, 2 * keep_y)).reshape(width, width, half)
    c, s = np.cos(theta), np.sin(theta)
    tables["phase"] = np.stack(
        [np.concatenate([c, c], -1), np.concatenate([s, -s], -1)], axis=1
    ).astype(np.float32)
    tz = turn * np.arange(depth).reshape(width, 1, slab, 1) / depth
    ty = turn * ky.reshape(1, 1, 1, -1) / rows
    tx = turn * kx.reshape(1, -1, 1, 1) / cols
    keeper = (np.abs(ky) < keep_y).reshape(1, 1, 1, -1)
    real = 1.0 + diffusion_number * (2 * np.cos(tz) + 2 * np.cos(ty) + 2 * np.cos(tx) - 6.0)
    imag = -(advect_zaxis * np.sin(tz) + advect_yaxis * np.sin(ty) + advect_xaxis * np.sin(tx))
    real = (real * keeper).reshape(width, keep_x, half)
    imag = (imag * keeper).reshape(width, keep_x, half)
    tables["symbol"] = np.stack(
        [np.concatenate([real, real], -1), np.concatenate([-imag, imag], -1)], axis=1
    ).astype(np.float32)
    tables["share"] = np.broadcast_to(
        np.where(kx == 0, 1.0, 2.0)[:, None] / (depth * rows * cols), (keep_x, 2 * half)
    ).astype(np.float32)
    return tables


def paired(width):
    return width & (width - 1) == 0


def target_of(place, step, width):
    return place ^ step if paired(width) else (place + step) % width


def source_of(place, step, width):
    return place ^ step if paired(width) else lax.rem(place - step + width, width)


def step_between(place, target, width):
    return place ^ target if paired(width) else lax.rem(target - place + width, width)


on_chip = pl.BlockSpec(memory_space=pltpu.VMEM)
off_chip = pl.BlockSpec(memory_space=pltpu.HBM)
in_scalars = pl.BlockSpec(memory_space=pltpu.SMEM)


def local_call(kernel, out_shape, operands, scratch=(), places=None, out_specs=None):
    specs = [in_scalars if operand.dtype == jnp.int32 else on_chip for operand in operands]
    for index, spec in (places or {}).items():
        specs[index] = spec
    if out_specs is None:
        out_specs = jax.tree.map(lambda _: on_chip, out_shape)
        out_shape = jax.tree.map(lambda out: pltpu.VMEM(out.shape, out.dtype), out_shape)
    return pl.pallas_call(
        kernel,
        out_shape=out_shape,
        in_specs=specs,
        out_specs=out_specs,
        scratch_shapes=list(scratch),
        compiler_params=pltpu.CompilerParams(vmem_limit_bytes=16 * 1024 * 1024),
    )(*operands)


def split(values):
    high = values.astype(jnp.bfloat16)
    low = (values - high.astype(jnp.float32)).astype(jnp.bfloat16)
    return high, low


def dot(left, right):
    return jnp.dot(left, right, preferred_element_type=jnp.float32)


def three_pass(values, high_table, low_table):
    count = values.shape[0]
    high, low = split(values)
    both = dot(jnp.concatenate([high, low]), high_table)
    return both[:count] + both[count:] + dot(high, low_table)


def along_x(cells, table):
    high, low = split(cells)
    both = lax.dot_general(
        table,
        jnp.concatenate([high, low], axis=1),
        (((1,), (1,)), ((), ())),
        preferred_element_type=jnp.float32,
    )
    count = table.shape[0] // 2
    return both[:count] + both[count:]


def by_field(waves, fields, keep):
    lanes = waves.shape[1] // fields
    real = [waves[:keep, f * lanes : (f + 1) * lanes] for f in range(fields)]
    imag = [waves[keep:, f * lanes : (f + 1) * lanes] for f in range(fields)]
    return jnp.concatenate(real), jnp.concatenate(imag)


def flux(state, sign):
    u, v, w, p, s = state
    c = (0.5 * sign) * (advect_zaxis + w)
    momentum = viscosity + c
    return [
        momentum * u,
        momentum * v,
        momentum * w + (0.5 * sign) * p,
        (0.5 * sign * compress_rate) * w,
        (diffusivity + c) * s,
    ]


def level_rate(state, source):
    u, v, _, p, _ = state
    rates = list(source)
    rows, cols = u.shape
    for axis, length, speed, velocity, lead in (
        (1, cols, advect_xaxis + u, u, 0),
        (0, rows, advect_yaxis + v, v, 1),
    ):
        half = 0.5 * speed
        for index, field in enumerate(state):
            if index == 3:
                plus = (0.5 * compress_rate) * velocity
                minus = -plus
            else:
                plus = (spread[index] + half) * field
                minus = (spread[index] - half) * field
            if index == lead:
                plus = plus + 0.5 * p
                minus = minus - 0.5 * p
            rates[index] = (
                rates[index] + pltpu.roll(plus, 1, axis) + pltpu.roll(minus, length - 1, axis)
            )
    for index, field in enumerate(state):
        if index != 3:
            rates[index] = rates[index] - (6.0 * spread[index]) * field
    return rates


def slab_rates(states, sources, put):
    slab = len(states)
    for layer in range(slab):
        rates = level_rate(states[layer](), sources[layer]())
        if layer > 0:
            rates = [r + g for r, g in zip(rates, flux(states[layer - 1](), 1.0))]
        if layer < slab - 1:
            rates = [r + g for r, g in zip(rates, flux(states[layer + 1](), -1.0))]
        put(layer, rates)


def reader(ref, layer):
    return lambda: [ref[f, layer] for f in range(ref.shape[0])]


def readers(ref):
    return [reader(ref, layer) for layer in range(ref.shape[1])]


def edge_layers_kernel(state_ref, up_ref, down_ref):
    fields, slab = state_ref.shape[:2]
    for f in range(fields):
        up_ref[f] = state_ref[f, slab - 1]
        down_ref[f] = state_ref[f, 0]


def first_rate_kernel(
    state_ref,
    source_ref,
    table_ref,
    rate_ref,
    waves_ref,
    rate_up_ref,
    rate_down_ref,
    feed_up_ref,
    feed_down_ref,
    *,
    step,
):
    fields, slab, rows, cols = state_ref.shape
    last = slab - 1

    def put(layer, rates):
        for f in range(fields):
            rate_ref[f, layer] = rates[f]
            if layer == last:
                rate_up_ref[f] = rates[f]
            if layer == 0:
                rate_down_ref[f] = rates[f]
        for inner, edge, out_ref, sign in (
            (last - 1, last, feed_up_ref, 1.0),
            (1, 0, feed_down_ref, -1.0),
        ):
            if layer == inner:
                second = [state_ref[f, layer] + step * rates[f] for f in range(fields)]
                for f, value in enumerate(flux(second, sign)):
                    out_ref[f] = source_ref[f, edge] + value

    slab_rates(readers(state_ref), readers(source_ref), put)
    keep = table_ref.shape[0] // 4
    cells = state_ref[...].reshape(fields * slab * rows, cols)
    real, imag = by_field(along_x(cells, table_ref[...]), fields, keep)
    lanes = real.shape[1]
    waves_ref[:, :lanes] = real
    waves_ref[:, lanes:] = imag


def second_rate_kernel(
    state_ref,
    rate_ref,
    source_ref,
    below_ref,
    above_ref,
    next_ref,
    stage_ref,
    *,
    step,
):
    fields, slab = state_ref.shape[:2]
    for layer in range(slab):
        rates = [rate_ref[f, layer] for f in range(fields)]
        for edge, came_ref, sign in ((0, below_ref, 1.0), (slab - 1, above_ref, -1.0)):
            if layer == edge:
                given = flux([came_ref[f] for f in range(fields)], sign)
                rates = [rate + gift for rate, gift in zip(rates, given)]
        for f in range(fields):
            stage_ref[f, layer] = state_ref[f, layer] + step * rates[f]

    def put(layer, rates):
        for f in range(fields):
            next_ref[f, layer] = rates[f]

    slab_rates(readers(stage_ref), readers(source_ref), put)


def third_rate_kernel(
    state_ref,
    second_ref,
    rate_ref,
    source_ref,
    below_ref,
    above_ref,
    below_rate_ref,
    above_rate_ref,
    base_ref,
    edge_rate_ref,
    edge_sum_ref,
    inner_sum_ref,
    third_ref,
    fourth_ref,
    *,
    steps,
    weight,
):
    fields, slab, rows, cols = state_ref.shape
    last = slab - 1
    ids = range(fields)
    blank = [jnp.zeros((rows, cols), jnp.float32)] * fields
    for layer in range(1, last):
        for f in ids:
            third_ref[f, layer] = state_ref[f, layer] + steps[1] * rate_ref[f, layer]
    for side, edge, came_ref, came_rate_ref, sign in (
        (0, 0, below_ref, below_rate_ref, 1.0),
        (1, last, above_ref, above_rate_ref, -1.0),
    ):
        outward = flux([state_ref[f, edge] for f in ids], -sign)
        second = [came_ref[f] + steps[0] * (came_rate_ref[f] + outward[f]) for f in ids]
        for f, value in enumerate(flux(second, sign)):
            third_ref[f, edge] = state_ref[f, edge] + steps[1] * (rate_ref[f, edge] + value)
        outward = flux([second_ref[f, edge] for f in ids], -sign)
        rates = level_rate(second, outward)
        for f in ids:
            base_ref[side, f] = came_ref[f] + steps[1] * rates[f]

    def put(layer, rates):
        for f in ids:
            if 0 < layer < last:
                fourth_ref[f, layer - 1] = state_ref[f, layer] + steps[2] * rates[f]
            else:
                edge_rate_ref[0 if layer == 0 else 1, f] = rates[f]

    slab_rates(readers(third_ref), readers(source_ref), put)

    def so_far(f, layer):
        return (
            2.0 * third_ref[f, layer] + second_ref[f, layer] - state_ref[f, layer]
        ) * (1.0 / 3.0)

    def put_inner(index, rates):
        for f in ids:
            inner_sum_ref[f, index] = (
                so_far(f, index + 1) + fourth_ref[f, index] * (1.0 / 3.0) + weight * rates[f]
            )

    slab_rates(readers(fourth_ref), readers(source_ref)[1:last], put_inner)
    for side, edge, inner, sign in ((0, 0, 0, -1.0), (1, last, slab - 3, 1.0)):
        for f, value in enumerate(flux([fourth_ref[f, inner] for f in ids], sign)):
            edge_sum_ref[side, f] = so_far(f, edge) + weight * (source_ref[f, edge] + value)


def forward_kernel(
    state_ref,
    base_ref,
    edge_rate_ref,
    edge_sum_ref,
    inner_sum_ref,
    below_ref,
    above_ref,
    shifted_ref,
    table_ref,
    high_ref,
    low_ref,
    phase_ref,
    out_ref,
    inner_ref,
    outer_ref,
    *,
    steps,
    weight,
):
    fields, slab, rows, cols = state_ref.shape
    last = slab - 1
    ids = range(fields)
    blank = [jnp.zeros((rows, cols), jnp.float32)] * fields
    inward = {}
    for side, edge, came_ref, sign in ((0, 0, below_ref, 1.0), (1, last, above_ref, -1.0)):
        third = [base_ref[side, f] + steps[1] * came_ref[f] for f in ids]
        given = flux(third, sign)
        fourth = [
            state_ref[f, edge] + steps[2] * (edge_rate_ref[side, f] + given[f]) for f in ids
        ]
        rates = level_rate(fourth, blank)
        for f in ids:
            inner_ref[f, edge] = (
                edge_sum_ref[side, f] + fourth[f] * (1.0 / 3.0) + weight * rates[f]
            )
        for f, value in enumerate(flux(fourth, -sign)):
            outer_ref[side, f] = weight * value
        inner = 1 if side == 0 else last - 1
        for f, value in enumerate(flux(fourth, sign)):
            earlier = inner_ref if inner in inward else inner_sum_ref
            shift = 0 if inner in inward else 1
            inner_ref[f, inner] = earlier[f, inner - shift] + weight * value
        inward[inner] = True
    for layer in range(1, last):
        if layer not in inward:
            for f in ids:
                inner_ref[f, layer] = inner_sum_ref[f, layer - 1]

    width = out_ref.shape[0]
    keep = table_ref.shape[0] // 4
    half = out_ref.shape[2] // 2
    place = lax.axis_index("space")
    table = table_ref[...]
    real, imag = by_field(
        along_x(inner_ref[...].reshape(fields * slab * rows, cols), table), fields, keep
    )
    outer_cells = jnp.concatenate(
        [outer_ref[side, f] for f in range(fields) for side in range(2)]
    )
    outer_real, outer_imag = by_field(along_x(outer_cells, table), fields, keep)
    shifted = shifted_ref[...]
    lanes = real.shape[1]
    left = jnp.concatenate(
        [real - shifted[:, :lanes], imag - shifted[:, lanes:], outer_real, outer_imag], axis=1
    )
    waves = three_pass(left, high_ref[...], low_ref[...])
    for group in range(width):
        block = waves[:, group * 2 * half : (group + 1) * 2 * half]
        turned = (
            block * phase_ref[place, 0, group, :][None, :]
            + pltpu.roll(block, half, 1) * phase_ref[place, 1, group, :][None, :]
        )
        out_ref[step_between(place, group, width)] = turned


def slot_of(moment, moment_id, slices):
    slot, stride = 0, 1
    for radix in radices(slices):
        ours = lax.rem(moment // stride, radix)
        slot = slot + lax.rem(ours + (radix - moment_id // stride % radix), radix) * stride
        stride *= radix
    return slot


def coarse_kernel(jump_ref, symbol_ref, share_ref, out_ref, kept_ref):
    slices, lines, lanes = jump_ref.shape
    keep = share_ref.shape[0]
    fields = lines // keep
    place = lax.axis_index("space")
    moment = lax.axis_index("tm")
    real = symbol_ref[place, 0]
    imag = symbol_ref[place, 1]
    share = share_ref[...]
    blank = jnp.zeros((keep, lanes), jnp.float32)
    current = [(blank, blank)] * fields
    sizes = []
    kept_ref[0] = jnp.zeros((lines, lanes), jnp.float32)
    for moment_id in range(slices):
        total = blank
        for value, _ in current:
            total = total + value * value
        sizes.append(jnp.sum(total * share, axis=0, keepdims=True))
        if moment_id == slices - 1:
            break
        slot = slot_of(moment, moment_id, slices)
        for f in range(fields):
            jump = jump_ref[slot, f * keep : (f + 1) * keep, :]
            value = jump + current[f][0]
            swapped = pltpu.roll(jump, lanes // 2, 1) + current[f][1]
            current[f] = (value * real + swapped * imag, swapped * real - value * imag)
            kept_ref[moment_id + 1, f * keep : (f + 1) * keep, :] = current[f][0]
    out_ref[:lines, :] = kept_ref[moment]
    sums = jnp.sum(jnp.concatenate(sizes), axis=1, keepdims=True)
    spare = out_ref.shape[0] - lines - slices
    if spare > 0:
        out_ref[lines + slices :, :] = jnp.zeros((spare, lanes), jnp.float32)
    out_ref[lines : lines + slices, :] = jnp.broadcast_to(sums, (slices, lanes))


def inverse_kernel(*refs, width, scales):
    block_refs = refs[:width]
    (
        fine_ref,
        below_ref,
        above_ref,
        high_ref,
        low_ref,
        table_ref,
        phase_ref,
        ends_ref,
        slice_ref,
        total_ref,
        order_ref,
        held_ref,
        norm_refs,
        sems,
        norm_sems,
    ) = refs[width:]
    fields, slab, rows, cols = fine_ref.shape
    place = lax.axis_index("space")
    moment = lax.axis_index("tm")
    lines, lanes = order_ref.shape[1:]
    keep = lines // fields
    sums = None
    for step in range(width):
        group = source_of(place, step, width)
        block = block_refs[step][:lines, :]
        order_ref[group] = (
            block * phase_ref[place, 0, group, :][None, :]
            - pltpu.roll(block, lanes // 2, 1) * phase_ref[place, 1, group, :][None, :]
        )
        part = block_refs[step][lines:, :]
        sums = part if sums is None else sums + part
    left = jnp.concatenate([order_ref[group] for group in range(width)], axis=1)
    waves = three_pass(left, high_ref[...], low_ref[...])
    count = slab * rows
    copies = []
    for f in range(fields):
        both = jnp.concatenate(
            [waves[f * keep : (f + 1) * keep, :count], waves[f * keep : (f + 1) * keep, count:]]
        )
        high, low = split(both)
        change = lax.dot_general(
            jnp.concatenate([high, low, high]),
            table_ref[...],
            (((0,), (0,)), ((), ())),
            preferred_element_type=jnp.float32,
        ).reshape(slab, rows, cols)
        for layer in range(slab):
            value = fine_ref[f, layer] + change[layer]
            if layer == 0:
                value = value + below_ref[f]
            if layer == slab - 1:
                value = value + above_ref[f]
            held_ref[f, layer] = value
        copies.append(pltpu.make_async_copy(held_ref.at[f], ends_ref.at[f], sems.at[f]))
        copies[-1].start()
    line = lax.broadcasted_iota(jnp.int32, sums.shape, 0)
    own = jnp.sum(jnp.where(line == moment, sums, 0.0), axis=0, keepdims=True)
    whole = jnp.sum(sums, axis=0, keepdims=True)
    norm_refs[0, 0] = jnp.sqrt(own * scales[0] + epsilon)[0, 0]
    norm_refs[1, 0] = jnp.sqrt(whole * scales[1] + epsilon)[0, 0]
    for side, out_ref in enumerate((slice_ref, total_ref)):
        copies.append(pltpu.make_async_copy(norm_refs.at[side], out_ref, norm_sems.at[side]))
        copies[-1].start()
    for copy in copies:
        copy.wait()


def halo(up, down):
    count = lax.axis_size("space")
    ups = [(i, (i + 1) % count) for i in range(count)]
    downs = [((i + 1) % count, i) for i in range(count)]
    return lax.ppermute(up, "space", ups), lax.ppermute(down, "space", downs)


def radices(count):
    parts = []
    while count % 4 == 0 and count > 4:
        parts.append(4)
        count //= 4
    if count > 1:
        parts.append(count)
    return sorted(parts)


def shards(starts, source):
    state_now = starts[0]
    fields, slab, rows, cols = state_now.shape
    width = lax.axis_size("space")
    slices = lax.axis_size("tm")
    depth = slab * width
    keep_y, keep_x = rows // 8, cols // 16
    lines, lanes = fields * keep_x, 2 * slab * 2 * keep_y
    tables = make_tables(slab, width, rows, cols)
    real = jnp.float32

    layer_shape = jax.ShapeDtypeStruct((fields, rows, cols), real)
    edge_shape = jax.ShapeDtypeStruct((2, fields, rows, cols), real)
    slab_shape = jax.ShapeDtypeStruct((fields, slab, rows, cols), real)
    inner_shape = jax.ShapeDtypeStruct((fields, slab - 2, rows, cols), real)
    steps = (0.5 * time_step, 0.5 * time_step, time_step)
    weight = time_step / 6.0

    up, down = local_call(edge_layers_kernel, (layer_shape, layer_shape), [state_now])
    below, above = halo(up, down)
    rates, start_waves, *given = local_call(
        functools.partial(first_rate_kernel, step=steps[0]),
        (
            slab_shape,
            jax.ShapeDtypeStruct((lines, 2 * slab * rows), real),
            *(layer_shape,) * 4,
        ),
        [state_now, source, tables["xforward"]],
    )
    below_rate, above_rate = halo(given[0], given[1])
    below_feed, above_feed = halo(given[2], given[3])
    next_waves = lax.ppermute(start_waves, "tm", [(i + 1, i) for i in range(slices - 1)])
    rates, second = local_call(
        functools.partial(second_rate_kernel, step=steps[0]),
        (slab_shape, slab_shape),
        [state_now, rates, source, below, above],
    )
    base, edge_rate, edge_sum, inner_sum = local_call(
        functools.partial(third_rate_kernel, steps=steps, weight=weight),
        (edge_shape, edge_shape, edge_shape, inner_shape),
        [state_now, second, rates, source, below, above, below_rate, above_rate],
        [
            pltpu.VMEM((fields, slab, rows, cols), real),
            pltpu.VMEM((fields, slab - 2, rows, cols), real),
        ],
    )
    waves, fine_inner, fine_outer = local_call(
        functools.partial(forward_kernel, steps=steps, weight=weight),
        (jax.ShapeDtypeStruct((width, lines, lanes), real), slab_shape, edge_shape),
        [
            state_now,
            base,
            edge_rate,
            edge_sum,
            inner_sum,
            below_feed,
            above_feed,
            next_waves,
            tables["xforward"],
            *tables["yzforward"],
            tables["phase"],
        ],
    )
    jump = waves[0]
    for step in range(1, width):
        part = lax.ppermute(
            waves[step], "space", [(i, target_of(i, step, width)) for i in range(width)]
        )
        jump = jump + part

    below, above = halo(fine_outer[1], fine_outer[0])

    jumps = jump[None]
    stride = 1
    for radix in radices(slices):
        parts = [jumps]
        for step in range(1, radix):
            pairs = []
            for i in range(slices):
                digit = i // stride % radix
                pairs.append((i, i + ((digit + step) % radix - digit) * stride))
            parts.append(lax.ppermute(jumps, "tm", pairs))
        jumps = jnp.concatenate(parts)
        stride *= radix

    message = local_call(
        coarse_kernel,
        jax.ShapeDtypeStruct((lines + -(-slices // 8) * 8, lanes), real),
        [jumps, tables["symbol"], tables["share"]],
        [pltpu.VMEM((slices, lines, lanes), real)],
    )
    blocks = [message]
    for step in range(1, width):
        blocks.append(
            lax.ppermute(message, "space", [(i, target_of(i, step, width)) for i in range(width)])
        )
    cells = fields * depth * rows * cols
    ends, slice_norm, total_norm = local_call(
        functools.partial(
            inverse_kernel, width=width, scales=(1.0 / cells, 1.0 / (cells * slices))
        ),
        (
            jax.ShapeDtypeStruct((fields, slab, rows, cols), real),
            jax.ShapeDtypeStruct((1,), real),
            jax.ShapeDtypeStruct((1,), real),
        ),
        [
            *blocks,
            fine_inner,
            below,
            above,
            *tables["yzinverse"],
            tables["xinverse"],
            tables["phase"],
        ],
        [
            pltpu.VMEM((width, lines, lanes), real),
            pltpu.VMEM((fields, slab, rows, cols), real),
            pltpu.SMEM((2, 1), real),
            pltpu.SemaphoreType.DMA((fields,)),
            pltpu.SemaphoreType.DMA((2,)),
        ],
        out_specs=(off_chip, off_chip, off_chip),
    )
    return ends[None], slice_norm, total_norm


def solution(mesh):
    in_specs = (P("tm", None, "space", None, None), P(None, "space", None, None))
    out_specs = (P("tm", None, "space", None, None), P("tm"), P())
    return jax.shard_map(shards, mesh=mesh, in_specs=in_specs, out_specs=out_specs, check_vma=False)
```

```python
import functools

import jax
import jax.numpy as jnp
import numpy as np
from jax import lax
from jax.experimental import pallas as pl
from jax.experimental.pallas import tpu as pltpu
from jax.sharding import PartitionSpec as P


viscosity = 0.08
diffusivity = 0.05
compress_rate = 0.25
time_step = 0.5
diffusion_number = 0.08
advect_xaxis = 0.2
advect_yaxis = 0.15
advect_zaxis = 0.1
epsilon = 1e-06
spread = (viscosity, viscosity, viscosity, None, diffusivity)


def hi_lo(table):
    table = np.asarray(table, np.float32)
    high = table.astype(jnp.bfloat16)
    low = (table - high.astype(np.float32)).astype(jnp.bfloat16)
    return high, low


@functools.lru_cache(None)
def make_tables(slab, width, rows, cols):
    depth = slab * width
    keep_y, keep_x = rows // 8, cols // 16
    ky = np.arange(2 * keep_y)
    ky = np.where(ky < keep_y, ky, ky - 2 * keep_y)
    kx = np.arange(keep_x)
    half = slab * 2 * keep_y
    turn = 2.0 * np.pi
    tables = {}
    angle = turn * kx[:, None] * np.arange(cols)[None, :] / cols
    wave = np.concatenate([np.cos(angle), -np.sin(angle)])
    high, low = hi_lo(wave)
    tables["xforward"] = np.block([[high, high], [low, np.zeros_like(low)]])
    weight = np.where(kx == 0, 1.0, 2.0)[:, None] / (depth * rows * cols)
    wave = np.concatenate([weight * np.cos(angle), -weight * np.sin(angle)])
    high, low = hi_lo(wave)
    tables["xinverse"] = np.concatenate([high, high, low])
    kz = np.arange(depth).reshape(width, 1, slab, 1)
    kyb = ky.reshape(1, 1, 1, -1)

    def joint(layers):
        layers = np.asarray(layers).reshape(-1, 1, 1, 1, 1, 1)
        cells = np.arange(rows).reshape(1, -1, 1, 1, 1, 1)
        theta = turn * (kz[None, None] * layers / depth + kyb[None, None] * cells / rows)
        return theta.reshape(-1, width, 1, slab, 2 * keep_y)

    def forward(layers):
        theta = joint(layers)
        c, s = np.cos(theta), np.sin(theta)
        real = np.concatenate([c, -s], axis=2)
        imag = np.concatenate([s, c], axis=2)
        count = theta.shape[0]
        return real.reshape(count, -1), imag.reshape(count, -1)

    inner = forward(range(slab))
    outer = forward([-1, slab])
    tables["yzforward"] = hi_lo(np.concatenate([inner[0], inner[1], outer[0], outer[1]]))
    theta = joint(range(slab))
    count = theta.shape[0]
    c, s = np.cos(theta), np.sin(theta)
    real = np.concatenate([c, -s], axis=2).reshape(count, -1).T
    imag = np.concatenate([s, c], axis=2).reshape(count, -1).T
    tables["yzinverse"] = hi_lo(np.concatenate([real, imag], axis=1))
    place = np.arange(width).reshape(-1, 1, 1, 1)
    theta = turn * ((kz.reshape(1, width, slab, 1) * place) % width) / width
    theta = np.broadcast_to(theta, (width, width, slab, 2 * keep_y)).reshape(width, width, half)
    c, s = np.cos(theta), np.sin(theta)
    tables["phase"] = np.stack(
        [np.concatenate([c, c], -1), np.concatenate([s, -s], -1)], axis=1
    ).astype(np.float32)
    tz = turn * np.arange(depth).reshape(width, 1, slab, 1) / depth
    ty = turn * ky.reshape(1, 1, 1, -1) / rows
    tx = turn * kx.reshape(1, -1, 1, 1) / cols
    keeper = (np.abs(ky) < keep_y).reshape(1, 1, 1, -1)
    real = 1.0 + diffusion_number * (2 * np.cos(tz) + 2 * np.cos(ty) + 2 * np.cos(tx) - 6.0)
    imag = -(advect_zaxis * np.sin(tz) + advect_yaxis * np.sin(ty) + advect_xaxis * np.sin(tx))
    real = (real * keeper).reshape(width, keep_x, half)
    imag = (imag * keeper).reshape(width, keep_x, half)
    tables["symbol"] = np.stack(
        [np.concatenate([real, real], -1), np.concatenate([-imag, imag], -1)], axis=1
    ).astype(np.float32)
    tables["share"] = np.broadcast_to(
        np.where(kx == 0, 1.0, 2.0)[:, None] / (depth * rows * cols), (keep_x, 2 * half)
    ).astype(np.float32)
    return tables


def paired(width):
    return width & (width - 1) == 0


def target_of(place, step, width):
    return place ^ step if paired(width) else (place + step) % width


def source_of(place, step, width):
    return place ^ step if paired(width) else lax.rem(place - step + width, width)


def step_between(place, target, width):
    return place ^ target if paired(width) else lax.rem(target - place + width, width)


on_chip = pl.BlockSpec(memory_space=pltpu.VMEM)
off_chip = pl.BlockSpec(memory_space=pltpu.HBM)
in_scalars = pl.BlockSpec(memory_space=pltpu.SMEM)


def local_call(kernel, out_shape, operands, scratch=(), places=None, out_specs=None):
    specs = [in_scalars if operand.dtype == jnp.int32 else on_chip for operand in operands]
    for index, spec in (places or {}).items():
        specs[index] = spec
    if out_specs is None:
        out_specs = jax.tree.map(lambda _: on_chip, out_shape)
        out_shape = jax.tree.map(lambda out: pltpu.VMEM(out.shape, out.dtype), out_shape)
    return pl.pallas_call(
        kernel,
        out_shape=out_shape,
        in_specs=specs,
        out_specs=out_specs,
        scratch_shapes=list(scratch),
        compiler_params=pltpu.CompilerParams(vmem_limit_bytes=16 * 1024 * 1024),
    )(*operands)


def split(values):
    high = values.astype(jnp.bfloat16)
    low = (values - high.astype(jnp.float32)).astype(jnp.bfloat16)
    return high, low


def dot(left, right):
    return jnp.dot(left, right, preferred_element_type=jnp.float32)


def three_pass(values, high_table, low_table):
    count = values.shape[0]
    high, low = split(values)
    both = dot(jnp.concatenate([high, low]), high_table)
    return both[:count] + both[count:] + dot(high, low_table)


def along_x(cells, table):
    high, low = split(cells)
    both = lax.dot_general(
        table,
        jnp.concatenate([high, low], axis=1),
        (((1,), (1,)), ((), ())),
        preferred_element_type=jnp.float32,
    )
    count = table.shape[0] // 2
    return both[:count] + both[count:]


def by_field(waves, fields, keep):
    lanes = waves.shape[1] // fields
    real = [waves[:keep, f * lanes : (f + 1) * lanes] for f in range(fields)]
    imag = [waves[keep:, f * lanes : (f + 1) * lanes] for f in range(fields)]
    return jnp.concatenate(real), jnp.concatenate(imag)


def flux(state, sign):
    u, v, w, p, s = state
    c = (0.5 * sign) * (advect_zaxis + w)
    momentum = viscosity + c
    return [
        momentum * u,
        momentum * v,
        momentum * w + (0.5 * sign) * p,
        (0.5 * sign * compress_rate) * w,
        (diffusivity + c) * s,
    ]


def level_rate(state, source):
    u, v, _, p, _ = state
    rates = list(source)
    rows, cols = u.shape
    for axis, length, speed, velocity, lead in (
        (1, cols, advect_xaxis + u, u, 0),
        (0, rows, advect_yaxis + v, v, 1),
    ):
        half = 0.5 * speed
        for index, field in enumerate(state):
            if index == 3:
                plus = (0.5 * compress_rate) * velocity
                minus = -plus
            else:
                plus = (spread[index] + half) * field
                minus = (spread[index] - half) * field
            if index == lead:
                plus = plus + 0.5 * p
                minus = minus - 0.5 * p
            rates[index] = (
                rates[index] + pltpu.roll(plus, 1, axis) + pltpu.roll(minus, length - 1, axis)
            )
    for index, field in enumerate(state):
        if index != 3:
            rates[index] = rates[index] - (6.0 * spread[index]) * field
    return rates


def slab_rates(states, sources, put):
    slab = len(states)
    for layer in range(slab):
        rates = level_rate(states[layer](), sources[layer]())
        if layer > 0:
            rates = [r + g for r, g in zip(rates, flux(states[layer - 1](), 1.0))]
        if layer < slab - 1:
            rates = [r + g for r, g in zip(rates, flux(states[layer + 1](), -1.0))]
        put(layer, rates)


def reader(ref, layer):
    return lambda: [ref[f, layer] for f in range(ref.shape[0])]


def readers(ref):
    return [reader(ref, layer) for layer in range(ref.shape[1])]


def edge_layers_kernel(state_ref, up_ref, down_ref):
    fields, slab = state_ref.shape[:2]
    for f in range(fields):
        up_ref[f] = state_ref[f, slab - 1]
        down_ref[f] = state_ref[f, 0]


def first_rate_kernel(
    state_ref,
    source_ref,
    table_ref,
    rate_ref,
    waves_ref,
    rate_up_ref,
    rate_down_ref,
    feed_up_ref,
    feed_down_ref,
    *,
    step,
):
    fields, slab, rows, cols = state_ref.shape
    last = slab - 1

    def put(layer, rates):
        for f in range(fields):
            rate_ref[f, layer] = rates[f]
            if layer == last:
                rate_up_ref[f] = rates[f]
            if layer == 0:
                rate_down_ref[f] = rates[f]
        for inner, edge, out_ref, sign in (
            (last - 1, last, feed_up_ref, 1.0),
            (1, 0, feed_down_ref, -1.0),
        ):
            if layer == inner:
                second = [state_ref[f, layer] + step * rates[f] for f in range(fields)]
                for f, value in enumerate(flux(second, sign)):
                    out_ref[f] = source_ref[f, edge] + value

    slab_rates(readers(state_ref), readers(source_ref), put)
    keep = table_ref.shape[0] // 4
    cells = state_ref[...].reshape(fields * slab * rows, cols)
    real, imag = by_field(along_x(cells, table_ref[...]), fields, keep)
    lanes = real.shape[1]
    waves_ref[:, :lanes] = real
    waves_ref[:, lanes:] = imag


def second_rate_kernel(
    state_ref,
    rate_ref,
    source_ref,
    below_ref,
    above_ref,
    next_ref,
    stage_ref,
    *,
    step,
):
    fields, slab = state_ref.shape[:2]
    for layer in range(slab):
        rates = [rate_ref[f, layer] for f in range(fields)]
        for edge, came_ref, sign in ((0, below_ref, 1.0), (slab - 1, above_ref, -1.0)):
            if layer == edge:
                given = flux([came_ref[f] for f in range(fields)], sign)
                rates = [rate + gift for rate, gift in zip(rates, given)]
        for f in range(fields):
            stage_ref[f, layer] = state_ref[f, layer] + step * rates[f]

    def put(layer, rates):
        for f in range(fields):
            next_ref[f, layer] = rates[f]

    slab_rates(readers(stage_ref), readers(source_ref), put)


def third_rate_kernel(
    state_ref,
    second_ref,
    rate_ref,
    source_ref,
    below_ref,
    above_ref,
    below_rate_ref,
    above_rate_ref,
    base_ref,
    edge_rate_ref,
    edge_sum_ref,
    inner_sum_ref,
    third_ref,
    fourth_ref,
    *,
    steps,
    weight,
):
    fields, slab, rows, cols = state_ref.shape
    last = slab - 1
    ids = range(fields)
    blank = [jnp.zeros((rows, cols), jnp.float32)] * fields
    for layer in range(1, last):
        for f in ids:
            third_ref[f, layer] = state_ref[f, layer] + steps[1] * rate_ref[f, layer]
    for side, edge, came_ref, came_rate_ref, sign in (
        (0, 0, below_ref, below_rate_ref, 1.0),
        (1, last, above_ref, above_rate_ref, -1.0),
    ):
        outward = flux([state_ref[f, edge] for f in ids], -sign)
        second = [came_ref[f] + steps[0] * (came_rate_ref[f] + outward[f]) for f in ids]
        for f, value in enumerate(flux(second, sign)):
            third_ref[f, edge] = state_ref[f, edge] + steps[1] * (rate_ref[f, edge] + value)
        outward = flux([second_ref[f, edge] for f in ids], -sign)
        rates = level_rate(second, outward)
        for f in ids:
            base_ref[side, f] = came_ref[f] + steps[1] * rates[f]

    def put(layer, rates):
        for f in ids:
            if 0 < layer < last:
                fourth_ref[f, layer - 1] = state_ref[f, layer] + steps[2] * rates[f]
            else:
                edge_rate_ref[0 if layer == 0 else 1, f] = rates[f]

    slab_rates(readers(third_ref), readers(source_ref), put)

    def so_far(f, layer):
        return (
            2.0 * third_ref[f, layer] + second_ref[f, layer] - state_ref[f, layer]
        ) * (1.0 / 3.0)

    def put_inner(index, rates):
        for f in ids:
            inner_sum_ref[f, index] = (
                so_far(f, index + 1) + fourth_ref[f, index] * (1.0 / 3.0) + weight * rates[f]
            )

    slab_rates(readers(fourth_ref), readers(source_ref)[1:last], put_inner)
    for side, edge, inner, sign in ((0, 0, 0, -1.0), (1, last, slab - 3, 1.0)):
        for f, value in enumerate(flux([fourth_ref[f, inner] for f in ids], sign)):
            edge_sum_ref[side, f] = so_far(f, edge) + weight * (source_ref[f, edge] + value)


def forward_kernel(
    state_ref,
    base_ref,
    edge_rate_ref,
    edge_sum_ref,
    inner_sum_ref,
    below_ref,
    above_ref,
    shifted_ref,
    table_ref,
    high_ref,
    low_ref,
    phase_ref,
    out_ref,
    inner_ref,
    outer_ref,
    *,
    steps,
    weight,
):
    fields, slab, rows, cols = state_ref.shape
    last = slab - 1
    ids = range(fields)
    blank = [jnp.zeros((rows, cols), jnp.float32)] * fields
    inward = {}
    for side, edge, came_ref, sign in ((0, 0, below_ref, 1.0), (1, last, above_ref, -1.0)):
        third = [base_ref[side, f] + steps[1] * came_ref[f] for f in ids]
        given = flux(third, sign)
        fourth = [
            state_ref[f, edge] + steps[2] * (edge_rate_ref[side, f] + given[f]) for f in ids
        ]
        rates = level_rate(fourth, blank)
        for f in ids:
            inner_ref[f, edge] = (
                edge_sum_ref[side, f] + fourth[f] * (1.0 / 3.0) + weight * rates[f]
            )
        for f, value in enumerate(flux(fourth, -sign)):
            outer_ref[side, f] = weight * value
        inner = 1 if side == 0 else last - 1
        for f, value in enumerate(flux(fourth, sign)):
            earlier = inner_ref if inner in inward else inner_sum_ref
            shift = 0 if inner in inward else 1
            inner_ref[f, inner] = earlier[f, inner - shift] + weight * value
        inward[inner] = True
    for layer in range(1, last):
        if layer not in inward:
            for f in ids:
                inner_ref[f, layer] = inner_sum_ref[f, layer - 1]

    width = out_ref.shape[0]
    keep = table_ref.shape[0] // 4
    half = out_ref.shape[2] // 2
    place = lax.axis_index("space")
    table = table_ref[...]
    real, imag = by_field(
        along_x(inner_ref[...].reshape(fields * slab * rows, cols), table), fields, keep
    )
    outer_cells = jnp.concatenate(
        [outer_ref[side, f] for f in range(fields) for side in range(2)]
    )
    outer_real, outer_imag = by_field(along_x(outer_cells, table), fields, keep)
    shifted = shifted_ref[...]
    lanes = real.shape[1]
    left = jnp.concatenate(
        [real - shifted[:, :lanes], imag - shifted[:, lanes:], outer_real, outer_imag], axis=1
    )
    waves = three_pass(left, high_ref[...], low_ref[...])
    for group in range(width):
        block = waves[:, group * 2 * half : (group + 1) * 2 * half]
        turned = (
            block * phase_ref[place, 0, group, :][None, :]
            + pltpu.roll(block, half, 1) * phase_ref[place, 1, group, :][None, :]
        )
        out_ref[step_between(place, group, width)] = turned


def coarse_kernel(jump_ref, symbol_ref, share_ref, out_ref, kept_ref):
    slices, lines, lanes = jump_ref.shape
    keep = share_ref.shape[0]
    fields = lines // keep
    place = lax.axis_index("space")
    moment = lax.axis_index("tm")
    real = symbol_ref[place, 0]
    imag = symbol_ref[place, 1]
    share = share_ref[...]
    blank = jnp.zeros((keep, lanes), jnp.float32)
    current = [(blank, blank)] * fields
    sizes = []
    kept_ref[0] = jnp.zeros((lines, lanes), jnp.float32)
    for moment_id in range(slices):
        total = blank
        for value, _ in current:
            total = total + value * value
        sizes.append(jnp.sum(total * share, axis=0, keepdims=True))
        if moment_id == slices - 1:
            break
        for f in range(fields):
            jump = jump_ref[moment_id, f * keep : (f + 1) * keep, :]
            value = jump + current[f][0]
            swapped = pltpu.roll(jump, lanes // 2, 1) + current[f][1]
            current[f] = (value * real + swapped * imag, swapped * real - value * imag)
            kept_ref[moment_id + 1, f * keep : (f + 1) * keep, :] = current[f][0]
    out_ref[:lines, :] = kept_ref[moment]
    sums = jnp.sum(jnp.concatenate(sizes), axis=1, keepdims=True)
    spare = out_ref.shape[0] - lines - slices
    if spare > 0:
        out_ref[lines + slices :, :] = jnp.zeros((spare, lanes), jnp.float32)
    out_ref[lines : lines + slices, :] = jnp.broadcast_to(sums, (slices, lanes))


def inverse_kernel(*refs, width, scales):
    block_refs = refs[:width]
    (
        fine_ref,
        below_ref,
        above_ref,
        high_ref,
        low_ref,
        table_ref,
        phase_ref,
        ends_ref,
        slice_ref,
        total_ref,
        order_ref,
        held_ref,
        norm_refs,
        sems,
        norm_sems,
    ) = refs[width:]
    fields, slab, rows, cols = fine_ref.shape
    place = lax.axis_index("space")
    moment = lax.axis_index("tm")
    lines, lanes = order_ref.shape[1:]
    keep = lines // fields
    sums = None
    for step in range(width):
        group = source_of(place, step, width)
        block = block_refs[step][:lines, :]
        order_ref[group] = (
            block * phase_ref[place, 0, group, :][None, :]
            - pltpu.roll(block, lanes // 2, 1) * phase_ref[place, 1, group, :][None, :]
        )
        part = block_refs[step][lines:, :]
        sums = part if sums is None else sums + part
    left = jnp.concatenate([order_ref[group] for group in range(width)], axis=1)
    waves = three_pass(left, high_ref[...], low_ref[...])
    count = slab * rows
    copies = []
    for f in range(fields):
        both = jnp.concatenate(
            [waves[f * keep : (f + 1) * keep, :count], waves[f * keep : (f + 1) * keep, count:]]
        )
        high, low = split(both)
        change = lax.dot_general(
            jnp.concatenate([high, low, high]),
            table_ref[...],
            (((0,), (0,)), ((), ())),
            preferred_element_type=jnp.float32,
        ).reshape(slab, rows, cols)
        for layer in range(slab):
            value = fine_ref[f, layer] + change[layer]
            if layer == 0:
                value = value + below_ref[f]
            if layer == slab - 1:
                value = value + above_ref[f]
            held_ref[f, layer] = value
        copies.append(pltpu.make_async_copy(held_ref.at[f], ends_ref.at[f], sems.at[f]))
        copies[-1].start()
    line = lax.broadcasted_iota(jnp.int32, sums.shape, 0)
    own = jnp.sum(jnp.where(line == moment, sums, 0.0), axis=0, keepdims=True)
    whole = jnp.sum(sums, axis=0, keepdims=True)
    norm_refs[0, 0] = jnp.sqrt(own * scales[0] + epsilon)[0, 0]
    norm_refs[1, 0] = jnp.sqrt(whole * scales[1] + epsilon)[0, 0]
    for side, out_ref in enumerate((slice_ref, total_ref)):
        copies.append(pltpu.make_async_copy(norm_refs.at[side], out_ref, norm_sems.at[side]))
        copies[-1].start()
    for copy in copies:
        copy.wait()


def halo(up, down):
    count = lax.axis_size("space")
    ups = [(i, (i + 1) % count) for i in range(count)]
    downs = [((i + 1) % count, i) for i in range(count)]
    return lax.ppermute(up, "space", ups), lax.ppermute(down, "space", downs)


def shards(starts, source):
    state_now = starts[0]
    fields, slab, rows, cols = state_now.shape
    width = lax.axis_size("space")
    slices = lax.axis_size("tm")
    depth = slab * width
    keep_y, keep_x = rows // 8, cols // 16
    lines, lanes = fields * keep_x, 2 * slab * 2 * keep_y
    tables = make_tables(slab, width, rows, cols)
    real = jnp.float32

    layer_shape = jax.ShapeDtypeStruct((fields, rows, cols), real)
    edge_shape = jax.ShapeDtypeStruct((2, fields, rows, cols), real)
    slab_shape = jax.ShapeDtypeStruct((fields, slab, rows, cols), real)
    inner_shape = jax.ShapeDtypeStruct((fields, slab - 2, rows, cols), real)
    steps = (0.5 * time_step, 0.5 * time_step, time_step)
    weight = time_step / 6.0

    up, down = local_call(edge_layers_kernel, (layer_shape, layer_shape), [state_now])
    below, above = halo(up, down)
    rates, start_waves, *given = local_call(
        functools.partial(first_rate_kernel, step=steps[0]),
        (
            slab_shape,
            jax.ShapeDtypeStruct((lines, 2 * slab * rows), real),
            *(layer_shape,) * 4,
        ),
        [state_now, source, tables["xforward"]],
    )
    below_rate, above_rate = halo(given[0], given[1])
    below_feed, above_feed = halo(given[2], given[3])
    next_waves = lax.ppermute(start_waves, "tm", [(i + 1, i) for i in range(slices - 1)])
    rates, second = local_call(
        functools.partial(second_rate_kernel, step=steps[0]),
        (slab_shape, slab_shape),
        [state_now, rates, source, below, above],
    )
    base, edge_rate, edge_sum, inner_sum = local_call(
        functools.partial(third_rate_kernel, steps=steps, weight=weight),
        (edge_shape, edge_shape, edge_shape, inner_shape),
        [state_now, second, rates, source, below, above, below_rate, above_rate],
        [
            pltpu.VMEM((fields, slab, rows, cols), real),
            pltpu.VMEM((fields, slab - 2, rows, cols), real),
        ],
    )
    waves, fine_inner, fine_outer = local_call(
        functools.partial(forward_kernel, steps=steps, weight=weight),
        (jax.ShapeDtypeStruct((width, lines, lanes), real), slab_shape, edge_shape),
        [
            state_now,
            base,
            edge_rate,
            edge_sum,
            inner_sum,
            below_feed,
            above_feed,
            next_waves,
            tables["xforward"],
            *tables["yzforward"],
            tables["phase"],
        ],
    )
    jump = waves[0]
    for step in range(1, width):
        part = lax.ppermute(
            waves[step], "space", [(i, target_of(i, step, width)) for i in range(width)]
        )
        jump = jump + part

    below, above = halo(fine_outer[1], fine_outer[0])

    jumps = lax.all_to_all(jnp.broadcast_to(jump, (slices, lines, lanes)), "tm", 0, 0, tiled=True)

    message = local_call(
        coarse_kernel,
        jax.ShapeDtypeStruct((lines + -(-slices // 8) * 8, lanes), real),
        [jumps, tables["symbol"], tables["share"]],
        [pltpu.VMEM((slices, lines, lanes), real)],
    )
    blocks = [message]
    for step in range(1, width):
        blocks.append(
            lax.ppermute(message, "space", [(i, target_of(i, step, width)) for i in range(width)])
        )
    cells = fields * depth * rows * cols
    ends, slice_norm, total_norm = local_call(
        functools.partial(
            inverse_kernel, width=width, scales=(1.0 / cells, 1.0 / (cells * slices))
        ),
        (
            jax.ShapeDtypeStruct((fields, slab, rows, cols), real),
            jax.ShapeDtypeStruct((1,), real),
            jax.ShapeDtypeStruct((1,), real),
        ),
        [
            *blocks,
            fine_inner,
            below,
            above,
            *tables["yzinverse"],
            tables["xinverse"],
            tables["phase"],
        ],
        [
            pltpu.VMEM((width, lines, lanes), real),
            pltpu.VMEM((fields, slab, rows, cols), real),
            pltpu.SMEM((2, 1), real),
            pltpu.SemaphoreType.DMA((fields,)),
            pltpu.SemaphoreType.DMA((2,)),
        ],
        out_specs=(off_chip, off_chip, off_chip),
    )
    return ends[None], slice_norm, total_norm


def solution(mesh):
    in_specs = (P("tm", None, "space", None, None), P(None, "space", None, None))
    out_specs = (P("tm", None, "space", None, None), P("tm"), P())
    return jax.shard_map(shards, mesh=mesh, in_specs=in_specs, out_specs=out_specs, check_vma=False)
```

```python
import functools

import jax
import jax.numpy as jnp
import numpy as np
from jax import lax
from jax.experimental import pallas as pl
from jax.experimental.pallas import tpu as pltpu
from jax.sharding import PartitionSpec as P


viscosity = 0.08
diffusivity = 0.05
compress_rate = 0.25
time_step = 0.5
diffusion_number = 0.08
advect_xaxis = 0.2
advect_yaxis = 0.15
advect_zaxis = 0.1
epsilon = 1e-06
spread = (viscosity, viscosity, viscosity, None, diffusivity)


def hi_lo(table):
    table = np.asarray(table, np.float32)
    high = table.astype(jnp.bfloat16)
    low = (table - high.astype(np.float32)).astype(jnp.bfloat16)
    return high, low


@functools.lru_cache(None)
def make_tables(slab, width, rows, cols):
    depth = slab * width
    keep_y, keep_x = rows // 8, cols // 16
    ky = np.arange(2 * keep_y)
    ky = np.where(ky < keep_y, ky, ky - 2 * keep_y)
    kx = np.arange(keep_x)
    half = slab * 2 * keep_y
    turn = 2.0 * np.pi
    tables = {}
    angle = turn * kx[:, None] * np.arange(cols)[None, :] / cols
    wave = np.concatenate([np.cos(angle), -np.sin(angle)])
    high, low = hi_lo(wave)
    tables["xforward"] = np.block([[high, high], [low, np.zeros_like(low)]])
    weight = np.where(kx == 0, 1.0, 2.0)[:, None] / (depth * rows * cols)
    wave = np.concatenate([weight * np.cos(angle), -weight * np.sin(angle)])
    high, low = hi_lo(wave)
    tables["xinverse"] = np.concatenate([high, high, low])
    kz = np.arange(depth).reshape(width, 1, slab, 1)
    kyb = ky.reshape(1, 1, 1, -1)

    def joint(layers):
        layers = np.asarray(layers).reshape(-1, 1, 1, 1, 1, 1)
        cells = np.arange(rows).reshape(1, -1, 1, 1, 1, 1)
        theta = turn * (kz[None, None] * layers / depth + kyb[None, None] * cells / rows)
        return theta.reshape(-1, width, 1, slab, 2 * keep_y)

    def forward(layers):
        theta = joint(layers)
        c, s = np.cos(theta), np.sin(theta)
        real = np.concatenate([c, -s], axis=2)
        imag = np.concatenate([s, c], axis=2)
        count = theta.shape[0]
        return real.reshape(count, -1), imag.reshape(count, -1)

    inner = forward(range(slab))
    outer = forward([-1, slab])
    tables["yzforward"] = hi_lo(np.concatenate([inner[0], inner[1], outer[0], outer[1]]))
    theta = joint(range(slab))
    count = theta.shape[0]
    c, s = np.cos(theta), np.sin(theta)
    real = np.concatenate([c, -s], axis=2).reshape(count, -1).T
    imag = np.concatenate([s, c], axis=2).reshape(count, -1).T
    tables["yzinverse"] = hi_lo(np.concatenate([real, imag], axis=1))
    place = np.arange(width).reshape(-1, 1, 1, 1)
    theta = turn * ((kz.reshape(1, width, slab, 1) * place) % width) / width
    theta = np.broadcast_to(theta, (width, width, slab, 2 * keep_y)).reshape(width, width, half)
    c, s = np.cos(theta), np.sin(theta)
    tables["phase"] = np.stack(
        [np.concatenate([c, c], -1), np.concatenate([s, -s], -1)], axis=1
    ).astype(np.float32)
    tz = turn * np.arange(depth).reshape(width, 1, slab, 1) / depth
    ty = turn * ky.reshape(1, 1, 1, -1) / rows
    tx = turn * kx.reshape(1, -1, 1, 1) / cols
    keeper = (np.abs(ky) < keep_y).reshape(1, 1, 1, -1)
    real = 1.0 + diffusion_number * (2 * np.cos(tz) + 2 * np.cos(ty) + 2 * np.cos(tx) - 6.0)
    imag = -(advect_zaxis * np.sin(tz) + advect_yaxis * np.sin(ty) + advect_xaxis * np.sin(tx))
    real = (real * keeper).reshape(width, keep_x, half)
    imag = (imag * keeper).reshape(width, keep_x, half)
    tables["symbol"] = np.stack(
        [np.concatenate([real, real], -1), np.concatenate([-imag, imag], -1)], axis=1
    ).astype(np.float32)
    tables["share"] = np.broadcast_to(
        np.where(kx == 0, 1.0, 2.0)[:, None] / (depth * rows * cols), (keep_x, 2 * half)
    ).astype(np.float32)
    return tables


def paired(width):
    return width & (width - 1) == 0


def target_of(place, step, width):
    return place ^ step if paired(width) else (place + step) % width


def source_of(place, step, width):
    return place ^ step if paired(width) else lax.rem(place - step + width, width)


def step_between(place, target, width):
    return place ^ target if paired(width) else lax.rem(target - place + width, width)


on_chip = pl.BlockSpec(memory_space=pltpu.VMEM)
off_chip = pl.BlockSpec(memory_space=pltpu.HBM)
in_scalars = pl.BlockSpec(memory_space=pltpu.SMEM)


def local_call(
    kernel, out_shape, operands, scratch=(), places=None, out_specs=None, aliases=None
):
    specs = [in_scalars if operand.dtype == jnp.int32 else on_chip for operand in operands]
    for index, spec in (places or {}).items():
        specs[index] = spec
    if out_specs is None:
        out_specs = jax.tree.map(lambda _: on_chip, out_shape)
        out_shape = jax.tree.map(lambda out: pltpu.VMEM(out.shape, out.dtype), out_shape)
    return pl.pallas_call(
        kernel,
        out_shape=out_shape,
        in_specs=specs,
        out_specs=out_specs,
        scratch_shapes=list(scratch),
        input_output_aliases=aliases or {},
        compiler_params=pltpu.CompilerParams(vmem_limit_bytes=16 * 1024 * 1024),
    )(*operands)


def split(values):
    high = values.astype(jnp.bfloat16)
    low = (values - high.astype(jnp.float32)).astype(jnp.bfloat16)
    return high, low


def dot(left, right):
    return jnp.dot(left, right, preferred_element_type=jnp.float32)


def three_pass(values, high_table, low_table):
    count = values.shape[0]
    high, low = split(values)
    both = dot(jnp.concatenate([high, low]), high_table)
    return both[:count] + both[count:] + dot(high, low_table)


def along_x(cells, table):
    high, low = split(cells)
    both = lax.dot_general(
        table,
        jnp.concatenate([high, low], axis=1),
        (((1,), (1,)), ((), ())),
        preferred_element_type=jnp.float32,
    )
    count = table.shape[0] // 2
    return both[:count] + both[count:]


def by_field(waves, fields, keep):
    lanes = waves.shape[1] // fields
    real = [waves[:keep, f * lanes : (f + 1) * lanes] for f in range(fields)]
    imag = [waves[keep:, f * lanes : (f + 1) * lanes] for f in range(fields)]
    return jnp.concatenate(real), jnp.concatenate(imag)


def flux(state, sign):
    u, v, w, p, s = state
    c = (0.5 * sign) * (advect_zaxis + w)
    momentum = viscosity + c
    return [
        momentum * u,
        momentum * v,
        momentum * w + (0.5 * sign) * p,
        (0.5 * sign * compress_rate) * w,
        (diffusivity + c) * s,
    ]


def level_rate(state, source):
    u, v, _, p, _ = state
    rates = list(source)
    rows, cols = u.shape
    for axis, length, speed, velocity, lead in (
        (1, cols, advect_xaxis + u, u, 0),
        (0, rows, advect_yaxis + v, v, 1),
    ):
        half = 0.5 * speed
        for index, field in enumerate(state):
            if index == 3:
                plus = (0.5 * compress_rate) * velocity
                minus = -plus
            else:
                plus = (spread[index] + half) * field
                minus = (spread[index] - half) * field
            if index == lead:
                plus = plus + 0.5 * p
                minus = minus - 0.5 * p
            rates[index] = (
                rates[index] + pltpu.roll(plus, 1, axis) + pltpu.roll(minus, length - 1, axis)
            )
    for index, field in enumerate(state):
        if index != 3:
            rates[index] = rates[index] - (6.0 * spread[index]) * field
    return rates


def slab_rates(states, sources, put):
    slab = len(states)
    for layer in range(slab):
        rates = level_rate(states[layer](), sources[layer]())
        if layer > 0:
            rates = [r + g for r, g in zip(rates, flux(states[layer - 1](), 1.0))]
        if layer < slab - 1:
            rates = [r + g for r, g in zip(rates, flux(states[layer + 1](), -1.0))]
        put(layer, rates)


def reader(ref, layer):
    return lambda: [ref[f, layer] for f in range(ref.shape[0])]


def readers(ref):
    return [reader(ref, layer) for layer in range(ref.shape[1])]


def edge_layers_kernel(state_ref, up_ref, down_ref):
    fields, slab = state_ref.shape[:2]
    for f in range(fields):
        up_ref[f] = state_ref[f, slab - 1]
        down_ref[f] = state_ref[f, 0]


def first_rate_kernel(
    state_ref,
    source_ref,
    table_ref,
    rate_ref,
    waves_ref,
    rate_up_ref,
    rate_down_ref,
    feed_up_ref,
    feed_down_ref,
    *,
    step,
):
    fields, slab, rows, cols = state_ref.shape
    last = slab - 1

    def put(layer, rates):
        for f in range(fields):
            rate_ref[f, layer] = rates[f]
            if layer == last:
                rate_up_ref[f] = rates[f]
            if layer == 0:
                rate_down_ref[f] = rates[f]
        for inner, edge, out_ref, sign in (
            (last - 1, last, feed_up_ref, 1.0),
            (1, 0, feed_down_ref, -1.0),
        ):
            if layer == inner:
                second = [state_ref[f, layer] + step * rates[f] for f in range(fields)]
                for f, value in enumerate(flux(second, sign)):
                    out_ref[f] = source_ref[f, edge] + value

    slab_rates(readers(state_ref), readers(source_ref), put)
    keep = table_ref.shape[0] // 4
    cells = state_ref[...].reshape(fields * slab * rows, cols)
    real, imag = by_field(along_x(cells, table_ref[...]), fields, keep)
    lanes = real.shape[1]
    waves_ref[:, :lanes] = real
    waves_ref[:, lanes:] = imag


def second_rate_kernel(
    state_ref,
    rate_ref,
    source_ref,
    below_ref,
    above_ref,
    next_ref,
    stage_ref,
    *,
    step,
):
    fields, slab = state_ref.shape[:2]
    for layer in range(slab):
        rates = [rate_ref[f, layer] for f in range(fields)]
        for edge, came_ref, sign in ((0, below_ref, 1.0), (slab - 1, above_ref, -1.0)):
            if layer == edge:
                given = flux([came_ref[f] for f in range(fields)], sign)
                rates = [rate + gift for rate, gift in zip(rates, given)]
        for f in range(fields):
            stage_ref[f, layer] = state_ref[f, layer] + step * rates[f]

    def put(layer, rates):
        for f in range(fields):
            next_ref[f, layer] = rates[f]

    slab_rates(readers(stage_ref), readers(source_ref), put)


def third_rate_kernel(
    state_ref,
    second_ref,
    rate_ref,
    source_ref,
    below_ref,
    above_ref,
    below_rate_ref,
    above_rate_ref,
    base_ref,
    edge_rate_ref,
    edge_sum_ref,
    inner_sum_ref,
    third_ref,
    fourth_ref,
    *,
    steps,
    weight,
):
    fields, slab, rows, cols = state_ref.shape
    last = slab - 1
    ids = range(fields)
    blank = [jnp.zeros((rows, cols), jnp.float32)] * fields
    for layer in range(1, last):
        for f in ids:
            third_ref[f, layer] = state_ref[f, layer] + steps[1] * rate_ref[f, layer]
    for side, edge, came_ref, came_rate_ref, sign in (
        (0, 0, below_ref, below_rate_ref, 1.0),
        (1, last, above_ref, above_rate_ref, -1.0),
    ):
        outward = flux([state_ref[f, edge] for f in ids], -sign)
        second = [came_ref[f] + steps[0] * (came_rate_ref[f] + outward[f]) for f in ids]
        for f, value in enumerate(flux(second, sign)):
            third_ref[f, edge] = state_ref[f, edge] + steps[1] * (rate_ref[f, edge] + value)
        outward = flux([second_ref[f, edge] for f in ids], -sign)
        rates = level_rate(second, outward)
        for f in ids:
            base_ref[side, f] = came_ref[f] + steps[1] * rates[f]

    def put(layer, rates):
        for f in ids:
            if 0 < layer < last:
                fourth_ref[f, layer - 1] = state_ref[f, layer] + steps[2] * rates[f]
            else:
                edge_rate_ref[0 if layer == 0 else 1, f] = rates[f]

    slab_rates(readers(third_ref), readers(source_ref), put)

    def so_far(f, layer):
        return (
            2.0 * third_ref[f, layer] + second_ref[f, layer] - state_ref[f, layer]
        ) * (1.0 / 3.0)

    def put_inner(index, rates):
        for f in ids:
            inner_sum_ref[f, index] = (
                so_far(f, index + 1) + fourth_ref[f, index] * (1.0 / 3.0) + weight * rates[f]
            )

    slab_rates(readers(fourth_ref), readers(source_ref)[1:last], put_inner)
    for side, edge, inner, sign in ((0, 0, 0, -1.0), (1, last, slab - 3, 1.0)):
        for f, value in enumerate(flux([fourth_ref[f, inner] for f in ids], sign)):
            edge_sum_ref[side, f] = so_far(f, edge) + weight * (source_ref[f, edge] + value)


def forward_kernel(
    state_ref,
    base_ref,
    edge_rate_ref,
    edge_sum_ref,
    inner_sum_ref,
    below_ref,
    above_ref,
    shifted_ref,
    table_ref,
    high_ref,
    low_ref,
    phase_ref,
    out_ref,
    inner_ref,
    outer_ref,
    *,
    steps,
    weight,
):
    fields, slab, rows, cols = state_ref.shape
    last = slab - 1
    ids = range(fields)
    blank = [jnp.zeros((rows, cols), jnp.float32)] * fields
    inward = {}
    for side, edge, came_ref, sign in ((0, 0, below_ref, 1.0), (1, last, above_ref, -1.0)):
        third = [base_ref[side, f] + steps[1] * came_ref[f] for f in ids]
        given = flux(third, sign)
        fourth = [
            state_ref[f, edge] + steps[2] * (edge_rate_ref[side, f] + given[f]) for f in ids
        ]
        rates = level_rate(fourth, blank)
        for f in ids:
            inner_ref[f, edge] = (
                edge_sum_ref[side, f] + fourth[f] * (1.0 / 3.0) + weight * rates[f]
            )
        for f, value in enumerate(flux(fourth, -sign)):
            outer_ref[side, f] = weight * value
        inner = 1 if side == 0 else last - 1
        for f, value in enumerate(flux(fourth, sign)):
            earlier = inner_ref if inner in inward else inner_sum_ref
            shift = 0 if inner in inward else 1
            inner_ref[f, inner] = earlier[f, inner - shift] + weight * value
        inward[inner] = True
    for layer in range(1, last):
        if layer not in inward:
            for f in ids:
                inner_ref[f, layer] = inner_sum_ref[f, layer - 1]

    width = out_ref.shape[0]
    keep = table_ref.shape[0] // 4
    half = out_ref.shape[2] // 2
    place = lax.axis_index("space")
    table = table_ref[...]
    real, imag = by_field(
        along_x(inner_ref[...].reshape(fields * slab * rows, cols), table), fields, keep
    )
    outer_cells = jnp.concatenate(
        [outer_ref[side, f] for f in range(fields) for side in range(2)]
    )
    outer_real, outer_imag = by_field(along_x(outer_cells, table), fields, keep)
    shifted = shifted_ref[...]
    lanes = real.shape[1]
    left = jnp.concatenate(
        [real - shifted[:, :lanes], imag - shifted[:, lanes:], outer_real, outer_imag], axis=1
    )
    waves = three_pass(left, high_ref[...], low_ref[...])
    for group in range(width):
        block = waves[:, group * 2 * half : (group + 1) * 2 * half]
        turned = (
            block * phase_ref[place, 0, group, :][None, :]
            + pltpu.roll(block, half, 1) * phase_ref[place, 1, group, :][None, :]
        )
        out_ref[step_between(place, group, width)] = turned


def coarse_kernel(jump_ref, symbol_ref, share_ref, out_ref, kept_ref):
    slices, lines, lanes = jump_ref.shape
    keep = share_ref.shape[0]
    fields = lines // keep
    place = lax.axis_index("space")
    moment = lax.axis_index("tm")
    real = symbol_ref[place, 0]
    imag = symbol_ref[place, 1]
    share = share_ref[...]
    blank = jnp.zeros((keep, lanes), jnp.float32)
    current = [(blank, blank)] * fields
    sizes = []
    kept_ref[0] = jnp.zeros((lines, lanes), jnp.float32)
    for moment_id in range(slices):
        total = blank
        for value, _ in current:
            total = total + value * value
        sizes.append(jnp.sum(total * share, axis=0, keepdims=True))
        if moment_id == slices - 1:
            break
        for f in range(fields):
            jump = jump_ref[moment_id, f * keep : (f + 1) * keep, :]
            value = jump + current[f][0]
            swapped = pltpu.roll(jump, lanes // 2, 1) + current[f][1]
            current[f] = (value * real + swapped * imag, swapped * real - value * imag)
            kept_ref[moment_id + 1, f * keep : (f + 1) * keep, :] = current[f][0]
    out_ref[:lines, :] = kept_ref[moment]
    sums = jnp.sum(jnp.concatenate(sizes), axis=1, keepdims=True)
    spare = out_ref.shape[0] - lines - slices
    if spare > 0:
        out_ref[lines + slices :, :] = jnp.zeros((spare, lanes), jnp.float32)
    out_ref[lines : lines + slices, :] = jnp.broadcast_to(sums, (slices, lanes))


def uncorrected_kernel(fine_ref, below_ref, above_ref, ends_ref, held_ref, sems):
    fields, slab = fine_ref.shape[:2]

    @pl.when(lax.axis_index("tm") == 0)
    def _():
        copies = []
        for f in range(fields):
            for layer in range(slab):
                value = fine_ref[f, layer]
                if layer == 0:
                    value = value + below_ref[f]
                if layer == slab - 1:
                    value = value + above_ref[f]
                held_ref[f, layer] = value
            copies.append(pltpu.make_async_copy(held_ref.at[f], ends_ref.at[f], sems.at[f]))
            copies[-1].start()
        for copy in copies:
            copy.wait()


def inverse_kernel(*refs, width, scales):
    block_refs = refs[:width]
    (
        fine_ref,
        below_ref,
        above_ref,
        high_ref,
        low_ref,
        table_ref,
        phase_ref,
        _,
        ends_ref,
        slice_ref,
        total_ref,
        order_ref,
        held_ref,
        norm_refs,
        sems,
        norm_sems,
    ) = refs[width:]
    fields, slab, rows, cols = fine_ref.shape
    place = lax.axis_index("space")
    moment = lax.axis_index("tm")
    lines, lanes = order_ref.shape[1:]
    keep = lines // fields

    sums = block_refs[0][lines:, :]
    for step in range(1, width):
        sums = sums + block_refs[step][lines:, :]
    line = lax.broadcasted_iota(jnp.int32, sums.shape, 0)
    own = jnp.sum(jnp.where(line == moment, sums, 0.0), axis=0, keepdims=True)
    whole = jnp.sum(sums, axis=0, keepdims=True)
    norm_refs[0, 0] = jnp.sqrt(own * scales[0] + epsilon)[0, 0]
    norm_refs[1, 0] = jnp.sqrt(whole * scales[1] + epsilon)[0, 0]
    norms = [
        pltpu.make_async_copy(norm_refs.at[side], out_ref, norm_sems.at[side])
        for side, out_ref in enumerate((slice_ref, total_ref))
    ]
    for copy in norms:
        copy.start()

    @pl.when(moment != 0)
    def _():
        for step in range(width):
            group = source_of(place, step, width)
            block = block_refs[step][:lines, :]
            order_ref[group] = (
                block * phase_ref[place, 0, group, :][None, :]
                - pltpu.roll(block, lanes // 2, 1) * phase_ref[place, 1, group, :][None, :]
            )
        left = jnp.concatenate([order_ref[group] for group in range(width)], axis=1)
        waves = three_pass(left, high_ref[...], low_ref[...])
        count = slab * rows
        copies = []
        for f in range(fields):
            own_waves = waves[f * keep : (f + 1) * keep]
            high, low = split(jnp.concatenate([own_waves[:, :count], own_waves[:, count:]]))
            change = lax.dot_general(
                jnp.concatenate([high, low, high]),
                table_ref[...],
                (((0,), (0,)), ((), ())),
                preferred_element_type=jnp.float32,
            ).reshape(slab, rows, cols)
            for layer in range(slab):
                value = fine_ref[f, layer] + change[layer]
                if layer == 0:
                    value = value + below_ref[f]
                if layer == slab - 1:
                    value = value + above_ref[f]
                held_ref[f, layer] = value
            copies.append(pltpu.make_async_copy(held_ref.at[f], ends_ref.at[f], sems.at[f]))
            copies[-1].start()
        for copy in copies:
            copy.wait()

    for copy in norms:
        copy.wait()


def halo(up, down):
    count = lax.axis_size("space")
    ups = [(i, (i + 1) % count) for i in range(count)]
    downs = [((i + 1) % count, i) for i in range(count)]
    return lax.ppermute(up, "space", ups), lax.ppermute(down, "space", downs)


def shards(starts, source):
    state_now = starts[0]
    fields, slab, rows, cols = state_now.shape
    width = lax.axis_size("space")
    slices = lax.axis_size("tm")
    depth = slab * width
    keep_y, keep_x = rows // 8, cols // 16
    lines, lanes = fields * keep_x, 2 * slab * 2 * keep_y
    tables = make_tables(slab, width, rows, cols)
    real = jnp.float32

    layer_shape = jax.ShapeDtypeStruct((fields, rows, cols), real)
    edge_shape = jax.ShapeDtypeStruct((2, fields, rows, cols), real)
    slab_shape = jax.ShapeDtypeStruct((fields, slab, rows, cols), real)
    inner_shape = jax.ShapeDtypeStruct((fields, slab - 2, rows, cols), real)
    steps = (0.5 * time_step, 0.5 * time_step, time_step)
    weight = time_step / 6.0

    up, down = local_call(edge_layers_kernel, (layer_shape, layer_shape), [state_now])
    below, above = halo(up, down)
    rates, start_waves, *given = local_call(
        functools.partial(first_rate_kernel, step=steps[0]),
        (
            slab_shape,
            jax.ShapeDtypeStruct((lines, 2 * slab * rows), real),
            *(layer_shape,) * 4,
        ),
        [state_now, source, tables["xforward"]],
    )
    below_rate, above_rate = halo(given[0], given[1])
    below_feed, above_feed = halo(given[2], given[3])
    next_waves = lax.ppermute(start_waves, "tm", [(i + 1, i) for i in range(slices - 1)])
    rates, second = local_call(
        functools.partial(second_rate_kernel, step=steps[0]),
        (slab_shape, slab_shape),
        [state_now, rates, source, below, above],
    )
    base, edge_rate, edge_sum, inner_sum = local_call(
        functools.partial(third_rate_kernel, steps=steps, weight=weight),
        (edge_shape, edge_shape, edge_shape, inner_shape),
        [state_now, second, rates, source, below, above, below_rate, above_rate],
        [
            pltpu.VMEM((fields, slab, rows, cols), real),
            pltpu.VMEM((fields, slab - 2, rows, cols), real),
        ],
    )
    waves, fine_inner, fine_outer = local_call(
        functools.partial(forward_kernel, steps=steps, weight=weight),
        (jax.ShapeDtypeStruct((width, lines, lanes), real), slab_shape, edge_shape),
        [
            state_now,
            base,
            edge_rate,
            edge_sum,
            inner_sum,
            below_feed,
            above_feed,
            next_waves,
            tables["xforward"],
            *tables["yzforward"],
            tables["phase"],
        ],
    )
    jump = waves[0]
    for step in range(1, width):
        part = lax.ppermute(
            waves[step], "space", [(i, target_of(i, step, width)) for i in range(width)]
        )
        jump = jump + part

    below, above = halo(fine_outer[1], fine_outer[0])

    jumps = lax.all_to_all(jnp.broadcast_to(jump, (slices, lines, lanes)), "tm", 0, 0, tiled=True)

    message = local_call(
        coarse_kernel,
        jax.ShapeDtypeStruct((lines + -(-slices // 8) * 8, lanes), real),
        [jumps, tables["symbol"], tables["share"]],
        [pltpu.VMEM((slices, lines, lanes), real)],
    )
    blocks = [message]
    for step in range(1, width):
        block = lax.ppermute(
            message, "space", [(i, target_of(i, step, width)) for i in range(width)]
        )
        blocks.append(block)
    whole_slab = pltpu.VMEM((fields, slab, rows, cols), real)
    ends = local_call(
        uncorrected_kernel,
        jax.ShapeDtypeStruct((fields, slab, rows, cols), real),
        [fine_inner, below, above],
        [whole_slab, pltpu.SemaphoreType.DMA((fields,))],
        out_specs=off_chip,
    )
    cells = fields * depth * rows * cols
    ends, slice_norm, total_norm = local_call(
        functools.partial(
            inverse_kernel, width=width, scales=(1.0 / cells, 1.0 / (cells * slices))
        ),
        (
            jax.ShapeDtypeStruct((fields, slab, rows, cols), real),
            jax.ShapeDtypeStruct((1,), real),
            jax.ShapeDtypeStruct((1,), real),
        ),
        [
            *blocks,
            fine_inner,
            below,
            above,
            *tables["yzinverse"],
            tables["xinverse"],
            tables["phase"],
            ends,
        ],
        [
            pltpu.VMEM((width, lines, lanes), real),
            whole_slab,
            pltpu.SMEM((2, 1), real),
            pltpu.SemaphoreType.DMA((fields,)),
            pltpu.SemaphoreType.DMA((2,)),
        ],
        places={width + 7: off_chip},
        out_specs=(off_chip, off_chip, off_chip),
        aliases={width + 7: 0},
    )
    return ends[None], slice_norm, total_norm


def solution(mesh):
    in_specs = (P("tm", None, "space", None, None), P(None, "space", None, None))
    out_specs = (P("tm", None, "space", None, None), P("tm"), P())
    return jax.shard_map(shards, mesh=mesh, in_specs=in_specs, out_specs=out_specs, check_vma=False)
```

```python
import functools

import jax
import jax.numpy as jnp
import numpy as np
from jax import lax
from jax.experimental import pallas as pl
from jax.experimental.pallas import tpu as pltpu
from jax.sharding import PartitionSpec as P


viscosity = 0.08
diffusivity = 0.05
compress_rate = 0.25
time_step = 0.5
diffusion_number = 0.08
advect_xaxis = 0.2
advect_yaxis = 0.15
advect_zaxis = 0.1
epsilon = 1e-06
spread = (viscosity, viscosity, viscosity, None, diffusivity)


def hi_lo(table):
    table = np.asarray(table, np.float32)
    high = table.astype(jnp.bfloat16)
    low = (table - high.astype(np.float32)).astype(jnp.bfloat16)
    return high, low


@functools.lru_cache(None)
def make_tables(slab, width, rows, cols):
    depth = slab * width
    keep_y, keep_x = rows // 8, cols // 16
    ky = np.arange(2 * keep_y)
    ky = np.where(ky < keep_y, ky, ky - 2 * keep_y)
    kx = np.arange(keep_x)
    half = slab * 2 * keep_y
    turn = 2.0 * np.pi
    tables = {}
    angle = turn * kx[:, None] * np.arange(cols)[None, :] / cols
    wave = np.concatenate([np.cos(angle), -np.sin(angle)])
    high, low = hi_lo(wave)
    tables["xforward"] = np.block([[high, high], [low, np.zeros_like(low)]])
    weight = np.where(kx == 0, 1.0, 2.0)[:, None] / (depth * rows * cols)
    wave = np.concatenate([weight * np.cos(angle), -weight * np.sin(angle)])
    high, low = hi_lo(wave)
    tables["xinverse"] = np.concatenate([high, high, low])
    kz = np.arange(depth).reshape(width, 1, slab, 1)
    kyb = ky.reshape(1, 1, 1, -1)

    def joint(layers):
        layers = np.asarray(layers).reshape(-1, 1, 1, 1, 1, 1)
        cells = np.arange(rows).reshape(1, -1, 1, 1, 1, 1)
        theta = turn * (kz[None, None] * layers / depth + kyb[None, None] * cells / rows)
        return theta.reshape(-1, width, 1, slab, 2 * keep_y)

    def forward(layers):
        theta = joint(layers)
        c, s = np.cos(theta), np.sin(theta)
        real = np.concatenate([c, -s], axis=2)
        imag = np.concatenate([s, c], axis=2)
        count = theta.shape[0]
        return real.reshape(count, -1), imag.reshape(count, -1)

    inner = forward(range(slab))
    outer = forward([-1, slab])
    tables["yzforward"] = hi_lo(np.concatenate([inner[0], inner[1], outer[0], outer[1]]))
    theta = turn * ky[None, :] * np.arange(rows)[:, None] / rows
    c, s = np.cos(theta), np.sin(theta)
    layers = np.eye(slab)

    def planes(block):
        return np.einsum("ab,yk->aybk", layers, block).reshape(slab * rows, -1)

    tables["yforward"] = hi_lo(np.block([[planes(c), -planes(s)], [planes(s), planes(c)]]))
    theta = turn * kz.reshape(1, width, slab) * np.arange(slab).reshape(-1, 1, 1) / depth
    c, s = np.cos(theta), np.sin(theta)
    modes = np.eye(2 * keep_y)

    def spread(real, imag):
        return np.einsum("zgrk,jl->zjgrkl", np.stack([real, imag], axis=2), modes).reshape(
            slab * 2 * keep_y, -1
        )

    tables["zforward"] = hi_lo(np.concatenate([spread(c, -s), spread(s, c)]))
    theta = joint(range(slab))
    count = theta.shape[0]
    c, s = np.cos(theta), np.sin(theta)
    real = np.concatenate([c, -s], axis=2).reshape(count, -1).T
    imag = np.concatenate([s, c], axis=2).reshape(count, -1).T
    tables["yzinverse"] = hi_lo(np.concatenate([real, imag], axis=1))
    place = np.arange(width).reshape(-1, 1, 1, 1)
    theta = turn * ((kz.reshape(1, width, slab, 1) * place) % width) / width
    theta = np.broadcast_to(theta, (width, width, slab, 2 * keep_y)).reshape(width, width, half)
    c, s = np.cos(theta), np.sin(theta)
    tables["phase"] = np.stack(
        [np.concatenate([c, c], -1), np.concatenate([s, -s], -1)], axis=1
    ).astype(np.float32)
    tz = turn * np.arange(depth).reshape(width, 1, slab, 1) / depth
    ty = turn * ky.reshape(1, 1, 1, -1) / rows
    tx = turn * kx.reshape(1, -1, 1, 1) / cols
    keeper = (np.abs(ky) < keep_y).reshape(1, 1, 1, -1)
    real = 1.0 + diffusion_number * (2 * np.cos(tz) + 2 * np.cos(ty) + 2 * np.cos(tx) - 6.0)
    imag = -(advect_zaxis * np.sin(tz) + advect_yaxis * np.sin(ty) + advect_xaxis * np.sin(tx))
    real = (real * keeper).reshape(width, keep_x, half)
    imag = (imag * keeper).reshape(width, keep_x, half)
    tables["symbol"] = np.stack(
        [np.concatenate([real, real], -1), np.concatenate([-imag, imag], -1)], axis=1
    ).astype(np.float32)
    tables["share"] = np.broadcast_to(
        np.where(kx == 0, 1.0, 2.0)[:, None] / (depth * rows * cols), (keep_x, 2 * half)
    ).astype(np.float32)
    return tables


def paired(width):
    return width & (width - 1) == 0


def target_of(place, step, width):
    return place ^ step if paired(width) else (place + step) % width


def source_of(place, step, width):
    return place ^ step if paired(width) else lax.rem(place - step + width, width)


def step_between(place, target, width):
    return place ^ target if paired(width) else lax.rem(target - place + width, width)


on_chip = pl.BlockSpec(memory_space=pltpu.VMEM)
off_chip = pl.BlockSpec(memory_space=pltpu.HBM)
in_scalars = pl.BlockSpec(memory_space=pltpu.SMEM)


def local_call(
    kernel, out_shape, operands, scratch=(), places=None, out_specs=None, aliases=None
):
    specs = [in_scalars if operand.dtype == jnp.int32 else on_chip for operand in operands]
    for index, spec in (places or {}).items():
        specs[index] = spec
    if out_specs is None:
        out_specs = jax.tree.map(lambda _: on_chip, out_shape)
        out_shape = jax.tree.map(lambda out: pltpu.VMEM(out.shape, out.dtype), out_shape)
    return pl.pallas_call(
        kernel,
        out_shape=out_shape,
        in_specs=specs,
        out_specs=out_specs,
        scratch_shapes=list(scratch),
        input_output_aliases=aliases or {},
        compiler_params=pltpu.CompilerParams(vmem_limit_bytes=16 * 1024 * 1024),
    )(*operands)


def split(values):
    high = values.astype(jnp.bfloat16)
    low = (values - high.astype(jnp.float32)).astype(jnp.bfloat16)
    return high, low


def dot(left, right):
    return jnp.dot(left, right, preferred_element_type=jnp.float32)


def three_pass(values, high_table, low_table):
    count = values.shape[0]
    high, low = split(values)
    both = dot(jnp.concatenate([high, low]), high_table)
    return both[:count] + both[count:] + dot(high, low_table)


def along_x(cells, table):
    high, low = split(cells)
    both = lax.dot_general(
        table,
        jnp.concatenate([high, low], axis=1),
        (((1,), (1,)), ((), ())),
        preferred_element_type=jnp.float32,
    )
    count = table.shape[0] // 2
    return both[:count] + both[count:]


def by_field(waves, fields, keep):
    lanes = waves.shape[1] // fields
    real = [waves[:keep, f * lanes : (f + 1) * lanes] for f in range(fields)]
    imag = [waves[keep:, f * lanes : (f + 1) * lanes] for f in range(fields)]
    return jnp.concatenate(real), jnp.concatenate(imag)


def flux(state, sign):
    u, v, w, p, s = state
    c = (0.5 * sign) * (advect_zaxis + w)
    momentum = viscosity + c
    return [
        momentum * u,
        momentum * v,
        momentum * w + (0.5 * sign) * p,
        (0.5 * sign * compress_rate) * w,
        (diffusivity + c) * s,
    ]


def level_rate(state, source):
    u, v, _, p, _ = state
    rates = list(source)
    rows, cols = u.shape
    for axis, length, speed, velocity, lead in (
        (1, cols, advect_xaxis + u, u, 0),
        (0, rows, advect_yaxis + v, v, 1),
    ):
        half = 0.5 * speed
        for index, field in enumerate(state):
            if index == 3:
                plus = (0.5 * compress_rate) * velocity
                minus = -plus
            else:
                plus = (spread[index] + half) * field
                minus = (spread[index] - half) * field
            if index == lead:
                plus = plus + 0.5 * p
                minus = minus - 0.5 * p
            rates[index] = (
                rates[index] + pltpu.roll(plus, 1, axis) + pltpu.roll(minus, length - 1, axis)
            )
    for index, field in enumerate(state):
        if index != 3:
            rates[index] = rates[index] - (6.0 * spread[index]) * field
    return rates


def slab_rates(states, sources, put):
    slab = len(states)
    for layer in range(slab):
        rates = level_rate(states[layer](), sources[layer]())
        if layer > 0:
            rates = [r + g for r, g in zip(rates, flux(states[layer - 1](), 1.0))]
        if layer < slab - 1:
            rates = [r + g for r, g in zip(rates, flux(states[layer + 1](), -1.0))]
        put(layer, rates)


def reader(ref, layer):
    return lambda: [ref[f, layer] for f in range(ref.shape[0])]


def readers(ref):
    return [reader(ref, layer) for layer in range(ref.shape[1])]


def edge_layers_kernel(state_ref, up_ref, down_ref):
    fields, slab = state_ref.shape[:2]
    for f in range(fields):
        up_ref[f] = state_ref[f, slab - 1]
        down_ref[f] = state_ref[f, 0]


def first_rate_kernel(
    state_ref,
    source_ref,
    table_ref,
    rate_ref,
    waves_ref,
    rate_up_ref,
    rate_down_ref,
    feed_up_ref,
    feed_down_ref,
    *,
    step,
):
    fields, slab, rows, cols = state_ref.shape
    last = slab - 1

    def put(layer, rates):
        for f in range(fields):
            rate_ref[f, layer] = rates[f]
            if layer == last:
                rate_up_ref[f] = rates[f]
            if layer == 0:
                rate_down_ref[f] = rates[f]
        for inner, edge, out_ref, sign in (
            (last - 1, last, feed_up_ref, 1.0),
            (1, 0, feed_down_ref, -1.0),
        ):
            if layer == inner:
                second = [state_ref[f, layer] + step * rates[f] for f in range(fields)]
                for f, value in enumerate(flux(second, sign)):
                    out_ref[f] = source_ref[f, edge] + value

    slab_rates(readers(state_ref), readers(source_ref), put)
    keep = table_ref.shape[0] // 4
    cells = state_ref[...].reshape(fields * slab * rows, cols)
    real, imag = by_field(along_x(cells, table_ref[...]), fields, keep)
    lanes = real.shape[1]
    waves_ref[:, :lanes] = real
    waves_ref[:, lanes:] = imag


def start_planes_kernel(waves_ref, high_ref, low_ref, out_ref):
    out_ref[...] = three_pass(waves_ref[...], high_ref[...], low_ref[...])


def second_rate_kernel(
    state_ref,
    rate_ref,
    source_ref,
    below_ref,
    above_ref,
    next_ref,
    stage_ref,
    *,
    step,
):
    fields, slab = state_ref.shape[:2]
    for layer in range(slab):
        rates = [rate_ref[f, layer] for f in range(fields)]
        for edge, came_ref, sign in ((0, below_ref, 1.0), (slab - 1, above_ref, -1.0)):
            if layer == edge:
                given = flux([came_ref[f] for f in range(fields)], sign)
                rates = [rate + gift for rate, gift in zip(rates, given)]
        for f in range(fields):
            stage_ref[f, layer] = state_ref[f, layer] + step * rates[f]

    def put(layer, rates):
        for f in range(fields):
            next_ref[f, layer] = rates[f]

    slab_rates(readers(stage_ref), readers(source_ref), put)


def third_rate_kernel(
    state_ref,
    second_ref,
    rate_ref,
    source_ref,
    below_ref,
    above_ref,
    below_rate_ref,
    above_rate_ref,
    base_ref,
    edge_rate_ref,
    edge_sum_ref,
    inner_sum_ref,
    third_ref,
    fourth_ref,
    *,
    steps,
    weight,
):
    fields, slab, rows, cols = state_ref.shape
    last = slab - 1
    ids = range(fields)
    blank = [jnp.zeros((rows, cols), jnp.float32)] * fields
    for layer in range(1, last):
        for f in ids:
            third_ref[f, layer] = state_ref[f, layer] + steps[1] * rate_ref[f, layer]
    for side, edge, came_ref, came_rate_ref, sign in (
        (0, 0, below_ref, below_rate_ref, 1.0),
        (1, last, above_ref, above_rate_ref, -1.0),
    ):
        outward = flux([state_ref[f, edge] for f in ids], -sign)
        second = [came_ref[f] + steps[0] * (came_rate_ref[f] + outward[f]) for f in ids]
        for f, value in enumerate(flux(second, sign)):
            third_ref[f, edge] = state_ref[f, edge] + steps[1] * (rate_ref[f, edge] + value)
        outward = flux([second_ref[f, edge] for f in ids], -sign)
        rates = level_rate(second, outward)
        for f in ids:
            base_ref[side, f] = came_ref[f] + steps[1] * rates[f]

    def put(layer, rates):
        for f in ids:
            if 0 < layer < last:
                fourth_ref[f, layer - 1] = state_ref[f, layer] + steps[2] * rates[f]
            else:
                edge_rate_ref[0 if layer == 0 else 1, f] = rates[f]

    slab_rates(readers(third_ref), readers(source_ref), put)

    def so_far(f, layer):
        return (
            2.0 * third_ref[f, layer] + second_ref[f, layer] - state_ref[f, layer]
        ) * (1.0 / 3.0)

    def put_inner(index, rates):
        for f in ids:
            inner_sum_ref[f, index] = (
                so_far(f, index + 1) + fourth_ref[f, index] * (1.0 / 3.0) + weight * rates[f]
            )

    slab_rates(readers(fourth_ref), readers(source_ref)[1:last], put_inner)
    for side, edge, inner, sign in ((0, 0, 0, -1.0), (1, last, slab - 3, 1.0)):
        for f, value in enumerate(flux([fourth_ref[f, inner] for f in ids], sign)):
            edge_sum_ref[side, f] = so_far(f, edge) + weight * (source_ref[f, edge] + value)


def forward_kernel(
    state_ref,
    base_ref,
    edge_rate_ref,
    edge_sum_ref,
    inner_sum_ref,
    below_ref,
    above_ref,
    shifted_ref,
    table_ref,
    high_ref,
    low_ref,
    shift_high_ref,
    shift_low_ref,
    phase_ref,
    out_ref,
    inner_ref,
    outer_ref,
    *,
    steps,
    weight,
):
    fields, slab, rows, cols = state_ref.shape
    last = slab - 1
    ids = range(fields)
    blank = [jnp.zeros((rows, cols), jnp.float32)] * fields
    inward = {}
    for side, edge, came_ref, sign in ((0, 0, below_ref, 1.0), (1, last, above_ref, -1.0)):
        third = [base_ref[side, f] + steps[1] * came_ref[f] for f in ids]
        given = flux(third, sign)
        fourth = [
            state_ref[f, edge] + steps[2] * (edge_rate_ref[side, f] + given[f]) for f in ids
        ]
        rates = level_rate(fourth, blank)
        for f in ids:
            inner_ref[f, edge] = (
                edge_sum_ref[side, f] + fourth[f] * (1.0 / 3.0) + weight * rates[f]
            )
        for f, value in enumerate(flux(fourth, -sign)):
            outer_ref[side, f] = weight * value
        inner = 1 if side == 0 else last - 1
        for f, value in enumerate(flux(fourth, sign)):
            earlier = inner_ref if inner in inward else inner_sum_ref
            shift = 0 if inner in inward else 1
            inner_ref[f, inner] = earlier[f, inner - shift] + weight * value
        inward[inner] = True
    for layer in range(1, last):
        if layer not in inward:
            for f in ids:
                inner_ref[f, layer] = inner_sum_ref[f, layer - 1]

    width = out_ref.shape[0]
    keep = table_ref.shape[0] // 4
    half = out_ref.shape[2] // 2
    place = lax.axis_index("space")
    table = table_ref[...]
    real, imag = by_field(
        along_x(inner_ref[...].reshape(fields * slab * rows, cols), table), fields, keep
    )
    outer_cells = jnp.concatenate(
        [outer_ref[side, f] for f in range(fields) for side in range(2)]
    )
    outer_real, outer_imag = by_field(along_x(outer_cells, table), fields, keep)
    left = jnp.concatenate([real, imag, outer_real, outer_imag], axis=1)
    waves = three_pass(left, high_ref[...], low_ref[...]) - three_pass(
        shifted_ref[...], shift_high_ref[...], shift_low_ref[...]
    )
    for group in range(width):
        block = waves[:, group * 2 * half : (group + 1) * 2 * half]
        turned = (
            block * phase_ref[place, 0, group, :][None, :]
            + pltpu.roll(block, half, 1) * phase_ref[place, 1, group, :][None, :]
        )
        out_ref[step_between(place, group, width)] = turned


def coarse_kernel(jump_ref, symbol_ref, share_ref, out_ref, kept_ref):
    slices, lines, lanes = jump_ref.shape
    keep = share_ref.shape[0]
    fields = lines // keep
    place = lax.axis_index("space")
    moment = lax.axis_index("tm")
    real = symbol_ref[place, 0]
    imag = symbol_ref[place, 1]
    share = share_ref[...]
    blank = jnp.zeros((keep, lanes), jnp.float32)
    current = [(blank, blank)] * fields
    sizes = []
    kept_ref[0] = jnp.zeros((lines, lanes), jnp.float32)
    for moment_id in range(slices):
        total = blank
        for value, _ in current:
            total = total + value * value
        sizes.append(jnp.sum(total * share, axis=0, keepdims=True))
        if moment_id == slices - 1:
            break
        for f in range(fields):
            jump = jump_ref[moment_id, f * keep : (f + 1) * keep, :]
            value = jump + current[f][0]
            swapped = pltpu.roll(jump, lanes // 2, 1) + current[f][1]
            current[f] = (value * real + swapped * imag, swapped * real - value * imag)
            kept_ref[moment_id + 1, f * keep : (f + 1) * keep, :] = current[f][0]
    out_ref[:lines, :] = kept_ref[moment]
    sums = jnp.sum(jnp.concatenate(sizes), axis=1, keepdims=True)
    spare = out_ref.shape[0] - lines - slices
    if spare > 0:
        out_ref[lines + slices :, :] = jnp.zeros((spare, lanes), jnp.float32)
    out_ref[lines : lines + slices, :] = jnp.broadcast_to(sums, (slices, lanes))


def uncorrected_kernel(fine_ref, below_ref, above_ref, ends_ref, held_ref, sems):
    fields, slab = fine_ref.shape[:2]

    @pl.when(lax.axis_index("tm") == 0)
    def _():
        copies = []
        for f in range(fields):
            for layer in range(slab):
                value = fine_ref[f, layer]
                if layer == 0:
                    value = value + below_ref[f]
                if layer == slab - 1:
                    value = value + above_ref[f]
                held_ref[f, layer] = value
            copies.append(pltpu.make_async_copy(held_ref.at[f], ends_ref.at[f], sems.at[f]))
            copies[-1].start()
        for copy in copies:
            copy.wait()


def inverse_kernel(*refs, width, scales):
    block_refs = refs[:width]
    (
        fine_ref,
        below_ref,
        above_ref,
        high_ref,
        low_ref,
        table_ref,
        phase_ref,
        _,
        ends_ref,
        slice_ref,
        total_ref,
        order_ref,
        held_ref,
        own_norm_ref,
        whole_norm_ref,
        sems,
        norm_sems,
    ) = refs[width:]
    fields, slab, rows, cols = fine_ref.shape
    place = lax.axis_index("space")
    moment = lax.axis_index("tm")
    lines, lanes = order_ref.shape[1:]
    keep = lines // fields

    sums = block_refs[0][lines:, :]
    for step in range(1, width):
        sums = sums + block_refs[step][lines:, :]
    line = lax.broadcasted_iota(jnp.int32, sums.shape, 0)
    own = jnp.sum(jnp.where(line == moment, sums, 0.0), axis=0, keepdims=True)
    whole = jnp.sum(sums, axis=0, keepdims=True)
    own_norm_ref[...] = jnp.sqrt(own * scales[0] + epsilon)[:, :1]
    whole_norm_ref[...] = jnp.sqrt(whole * scales[1] + epsilon)[:, :1]
    norms = [
        pltpu.make_async_copy(own_norm_ref, slice_ref, norm_sems.at[0]),
        pltpu.make_async_copy(whole_norm_ref, total_ref, norm_sems.at[1]),
    ]
    for copy in norms:
        copy.start()

    @pl.when(moment != 0)
    def _():
        for step in range(width):
            group = source_of(place, step, width)
            block = block_refs[step][:lines, :]
            order_ref[group] = (
                block * phase_ref[place, 0, group, :][None, :]
                - pltpu.roll(block, lanes // 2, 1) * phase_ref[place, 1, group, :][None, :]
            )
        left = jnp.concatenate([order_ref[group] for group in range(width)], axis=1)
        waves = three_pass(left, high_ref[...], low_ref[...])
        count = slab * rows
        copies = []
        for f in range(fields):
            own_waves = waves[f * keep : (f + 1) * keep]
            high, low = split(jnp.concatenate([own_waves[:, :count], own_waves[:, count:]]))
            change = lax.dot_general(
                jnp.concatenate([high, low, high]),
                table_ref[...],
                (((0,), (0,)), ((), ())),
                preferred_element_type=jnp.float32,
            ).reshape(slab, rows, cols)
            for layer in range(slab):
                value = fine_ref[f, layer] + change[layer]
                if layer == 0:
                    value = value + below_ref[f]
                if layer == slab - 1:
                    value = value + above_ref[f]
                held_ref[f, layer] = value
            copies.append(pltpu.make_async_copy(held_ref.at[f], ends_ref.at[f], sems.at[f]))
            copies[-1].start()
        for copy in copies:
            copy.wait()

    for copy in norms:
        copy.wait()


def halo(up, down):
    count = lax.axis_size("space")
    ups = [(i, (i + 1) % count) for i in range(count)]
    downs = [((i + 1) % count, i) for i in range(count)]
    below = lax.ppermute(up, "space", ups)
    above = lax.ppermute(down, "space", downs)
    return below, above


def shards(starts, source):
    state_now = starts[0]
    fields, slab, rows, cols = state_now.shape
    width = lax.axis_size("space")
    slices = lax.axis_size("tm")
    depth = slab * width
    keep_y, keep_x = rows // 8, cols // 16
    lines, lanes = fields * keep_x, 2 * slab * 2 * keep_y
    tables = make_tables(slab, width, rows, cols)
    real = jnp.float32

    layer_shape = jax.ShapeDtypeStruct((fields, rows, cols), real)
    edge_shape = jax.ShapeDtypeStruct((2, fields, rows, cols), real)
    slab_shape = jax.ShapeDtypeStruct((fields, slab, rows, cols), real)
    inner_shape = jax.ShapeDtypeStruct((fields, slab - 2, rows, cols), real)
    steps = (0.5 * time_step, 0.5 * time_step, time_step)
    weight = time_step / 6.0

    up, down = local_call(edge_layers_kernel, (layer_shape, layer_shape), [state_now])
    below, above = halo(up, down)
    rates, start_waves, *given = local_call(
        functools.partial(first_rate_kernel, step=steps[0]),
        (
            slab_shape,
            jax.ShapeDtypeStruct((lines, 2 * slab * rows), real),
            *(layer_shape,) * 4,
        ),
        [state_now, source, tables["xforward"]],
    )
    below_rate, above_rate = halo(given[0], given[1])
    below_feed, above_feed = halo(given[2], given[3])
    start_planes = local_call(
        start_planes_kernel,
        jax.ShapeDtypeStruct((lines, lanes), real),
        [start_waves, *tables["yforward"]],
    )
    next_waves = lax.ppermute(start_planes, "tm", [(i + 1, i) for i in range(slices - 1)])
    rates, second = local_call(
        functools.partial(second_rate_kernel, step=steps[0]),
        (slab_shape, slab_shape),
        [state_now, rates, source, below, above],
    )
    base, edge_rate, edge_sum, inner_sum = local_call(
        functools.partial(third_rate_kernel, steps=steps, weight=weight),
        (edge_shape, edge_shape, edge_shape, inner_shape),
        [state_now, second, rates, source, below, above, below_rate, above_rate],
        [
            pltpu.VMEM((fields, slab, rows, cols), real),
            pltpu.VMEM((fields, slab - 2, rows, cols), real),
        ],
    )
    waves, fine_inner, fine_outer = local_call(
        functools.partial(forward_kernel, steps=steps, weight=weight),
        (jax.ShapeDtypeStruct((width, lines, lanes), real), slab_shape, edge_shape),
        [
            state_now,
            base,
            edge_rate,
            edge_sum,
            inner_sum,
            below_feed,
            above_feed,
            next_waves,
            tables["xforward"],
            *tables["yzforward"],
            *tables["zforward"],
            tables["phase"],
        ],
    )
    jump = waves[0]
    for step in range(1, width):
        part = lax.ppermute(
            waves[step], "space", [(i, target_of(i, step, width)) for i in range(width)]
        )
        jump = jump + part

    below, above = halo(fine_outer[1], fine_outer[0])

    jumps = lax.all_to_all(jnp.broadcast_to(jump, (slices, lines, lanes)), "tm", 0, 0, tiled=True)

    message = local_call(
        coarse_kernel,
        jax.ShapeDtypeStruct((lines + -(-slices // 8) * 8, lanes), real),
        [jumps, tables["symbol"], tables["share"]],
        [pltpu.VMEM((slices, lines, lanes), real)],
    )
    blocks = [message]
    for step in range(1, width):
        block = lax.ppermute(
            message, "space", [(i, target_of(i, step, width)) for i in range(width)]
        )
        blocks.append(block)
    whole_slab = pltpu.VMEM((fields, slab, rows, cols), real)
    ends = local_call(
        uncorrected_kernel,
        jax.ShapeDtypeStruct((fields, slab, rows, cols), real),
        [fine_inner, below, above],
        [whole_slab, pltpu.SemaphoreType.DMA((fields,))],
        out_specs=off_chip,
    )
    cells = fields * depth * rows * cols
    ends, slice_norm, total_norm = local_call(
        functools.partial(
            inverse_kernel, width=width, scales=(1.0 / cells, 1.0 / (cells * slices))
        ),
        (
            jax.ShapeDtypeStruct((fields, slab, rows, cols), real),
            jax.ShapeDtypeStruct((1, 1), real),
            jax.ShapeDtypeStruct((1, 1), real),
        ),
        [
            *blocks,
            fine_inner,
            below,
            above,
            *tables["yzinverse"],
            tables["xinverse"],
            tables["phase"],
            ends,
        ],
        [
            pltpu.VMEM((width, lines, lanes), real),
            whole_slab,
            pltpu.VMEM((1, 1), real),
            pltpu.VMEM((1, 1), real),
            pltpu.SemaphoreType.DMA((fields,)),
            pltpu.SemaphoreType.DMA((2,)),
        ],
        places={width + 7: off_chip},
        out_specs=(off_chip, off_chip, off_chip),
        aliases={width + 7: 0},
    )
    return ends[None], slice_norm[0], total_norm[0]


def solution(mesh):
    in_specs = (P("tm", None, "space", None, None), P(None, "space", None, None))
    out_specs = (P("tm", None, "space", None, None), P("tm"), P())
    return jax.shard_map(shards, mesh=mesh, in_specs=in_specs, out_specs=out_specs, check_vma=False)
```

```python
import functools

import jax
import jax.numpy as jnp
import numpy as np
from jax import lax
from jax.experimental import pallas as pl
from jax.experimental.pallas import tpu as pltpu
from jax.sharding import PartitionSpec as P


viscosity = 0.08
diffusivity = 0.05
compress_rate = 0.25
time_step = 0.5
diffusion_number = 0.08
advect_xaxis = 0.2
advect_yaxis = 0.15
advect_zaxis = 0.1
epsilon = 1e-06
spread = (viscosity, viscosity, viscosity, None, diffusivity)


def hi_lo(table):
    table = np.asarray(table, np.float32)
    high = table.astype(jnp.bfloat16)
    low = (table - high.astype(np.float32)).astype(jnp.bfloat16)
    return high, low


@functools.lru_cache(None)
def make_tables(slab, width, rows, cols):
    depth = slab * width
    keep_y, keep_x = rows // 8, cols // 16
    ky = np.arange(2 * keep_y)
    ky = np.where(ky < keep_y, ky, ky - 2 * keep_y)
    kx = np.arange(keep_x)
    half = slab * 2 * keep_y
    turn = 2.0 * np.pi
    tables = {}
    angle = turn * kx[:, None] * np.arange(cols)[None, :] / cols
    wave = np.concatenate([np.cos(angle), -np.sin(angle)])
    high, low = hi_lo(wave)
    tables["xforward"] = np.block([[high, high], [low, np.zeros_like(low)]])
    weight = np.where(kx == 0, 1.0, 2.0)[:, None] / (depth * rows * cols)
    wave = np.concatenate([weight * np.cos(angle), -weight * np.sin(angle)])
    high, low = hi_lo(wave)
    tables["xinverse"] = np.concatenate([high, high, low])
    kz = np.arange(depth).reshape(width, 1, slab, 1)
    kyb = ky.reshape(1, 1, 1, -1)

    def joint(layers):
        layers = np.asarray(layers).reshape(-1, 1, 1, 1, 1, 1)
        cells = np.arange(rows).reshape(1, -1, 1, 1, 1, 1)
        theta = turn * (kz[None, None] * layers / depth + kyb[None, None] * cells / rows)
        return theta.reshape(-1, width, 1, slab, 2 * keep_y)

    def forward(layers):
        theta = joint(layers)
        c, s = np.cos(theta), np.sin(theta)
        real = np.concatenate([c, -s], axis=2)
        imag = np.concatenate([s, c], axis=2)
        count = theta.shape[0]
        return real.reshape(count, -1), imag.reshape(count, -1)

    inner = forward(range(slab))
    outer = forward([-1, slab])
    tables["yzforward"] = hi_lo(np.concatenate([inner[0], inner[1], outer[0], outer[1]]))
    theta = joint(range(slab))
    count = theta.shape[0]
    c, s = np.cos(theta), np.sin(theta)
    real = np.concatenate([c, -s], axis=2).reshape(count, -1).T
    imag = np.concatenate([s, c], axis=2).reshape(count, -1).T
    both = np.concatenate([real, imag], axis=1)
    both[np.arange(both.shape[0]) % (2 * keep_y) == keep_y] = 0.0
    tables["yzinverse"] = hi_lo(both)
    place = np.arange(width).reshape(-1, 1, 1, 1)
    theta = turn * ((kz.reshape(1, width, slab, 1) * place) % width) / width
    theta = np.broadcast_to(theta, (width, width, slab, 2 * keep_y)).reshape(width, width, half)
    c, s = np.cos(theta), np.sin(theta)
    tables["phase"] = np.stack(
        [np.concatenate([c, c], -1), np.concatenate([s, -s], -1)], axis=1
    ).astype(np.float32)
    tz = turn * np.arange(depth).reshape(width, 1, slab, 1) / depth
    ty = turn * ky.reshape(1, 1, 1, -1) / rows
    tx = turn * kx.reshape(1, -1, 1, 1) / cols
    keeper = (np.abs(ky) < keep_y).reshape(1, 1, 1, -1)
    real = 1.0 + diffusion_number * (2 * np.cos(tz) + 2 * np.cos(ty) + 2 * np.cos(tx) - 6.0)
    imag = -(advect_zaxis * np.sin(tz) + advect_yaxis * np.sin(ty) + advect_xaxis * np.sin(tx))
    real = (real * keeper).reshape(width, keep_x, half)
    imag = (imag * keeper).reshape(width, keep_x, half)
    tables["symbol"] = np.stack(
        [np.concatenate([real, real], -1), np.concatenate([-imag, imag], -1)], axis=1
    ).astype(np.float32)
    tables["share"] = np.broadcast_to(
        np.where(kx == 0, 1.0, 2.0)[:, None] / (depth * rows * cols), (keep_x, 2 * half)
    ).astype(np.float32)
    return tables


def paired(width):
    return width & (width - 1) == 0


def target_of(place, step, width):
    return place ^ step if paired(width) else (place + step) % width


def source_of(place, step, width):
    return place ^ step if paired(width) else lax.rem(place - step + width, width)


def step_between(place, target, width):
    return place ^ target if paired(width) else lax.rem(target - place + width, width)


on_chip = pl.BlockSpec(memory_space=pltpu.VMEM)
off_chip = pl.BlockSpec(memory_space=pltpu.HBM)
in_scalars = pl.BlockSpec(memory_space=pltpu.SMEM)


def local_call(
    kernel, out_shape, operands, scratch=(), places=None, out_specs=None, aliases=None
):
    specs = [in_scalars if operand.dtype == jnp.int32 else on_chip for operand in operands]
    for index, spec in (places or {}).items():
        specs[index] = spec
    if out_specs is None:
        out_specs = jax.tree.map(lambda _: on_chip, out_shape)
        out_shape = jax.tree.map(lambda out: pltpu.VMEM(out.shape, out.dtype), out_shape)
    return pl.pallas_call(
        kernel,
        out_shape=out_shape,
        in_specs=specs,
        out_specs=out_specs,
        scratch_shapes=list(scratch),
        input_output_aliases=aliases or {},
        compiler_params=pltpu.CompilerParams(vmem_limit_bytes=16 * 1024 * 1024),
    )(*operands)


def split(values):
    high = values.astype(jnp.bfloat16)
    low = (values - high.astype(jnp.float32)).astype(jnp.bfloat16)
    return high, low


def dot(left, right):
    return jnp.dot(left, right, preferred_element_type=jnp.float32)


def three_pass(values, high_table, low_table):
    count = values.shape[0]
    high, low = split(values)
    both = dot(jnp.concatenate([high, low]), high_table)
    return both[:count] + both[count:] + dot(high, low_table)


def along_x(cells, table):
    high, low = split(cells)
    both = lax.dot_general(
        table,
        jnp.concatenate([high, low], axis=1),
        (((1,), (1,)), ((), ())),
        preferred_element_type=jnp.float32,
    )
    count = table.shape[0] // 2
    return both[:count] + both[count:]


def by_field(waves, fields, keep):
    lanes = waves.shape[1] // fields
    real = [waves[:keep, f * lanes : (f + 1) * lanes] for f in range(fields)]
    imag = [waves[keep:, f * lanes : (f + 1) * lanes] for f in range(fields)]
    return jnp.concatenate(real), jnp.concatenate(imag)


def flux(state, sign):
    u, v, w, p, s = state
    c = (0.5 * sign) * (advect_zaxis + w)
    momentum = viscosity + c
    return [
        momentum * u,
        momentum * v,
        momentum * w + (0.5 * sign) * p,
        (0.5 * sign * compress_rate) * w,
        (diffusivity + c) * s,
    ]


def level_rate(state, source):
    u, v, _, p, _ = state
    rates = list(source)
    rows, cols = u.shape
    for axis, length, speed, velocity, lead in (
        (1, cols, advect_xaxis + u, u, 0),
        (0, rows, advect_yaxis + v, v, 1),
    ):
        half = 0.5 * speed
        for index, field in enumerate(state):
            if index == 3:
                plus = (0.5 * compress_rate) * velocity
                minus = -plus
            else:
                plus = (spread[index] + half) * field
                minus = (spread[index] - half) * field
            if index == lead:
                plus = plus + 0.5 * p
                minus = minus - 0.5 * p
            rates[index] = (
                rates[index] + pltpu.roll(plus, 1, axis) + pltpu.roll(minus, length - 1, axis)
            )
    for index, field in enumerate(state):
        if index != 3:
            rates[index] = rates[index] - (6.0 * spread[index]) * field
    return rates


def slab_rates(states, sources, put):
    slab = len(states)
    for layer in range(slab):
        rates = level_rate(states[layer](), sources[layer]())
        if layer > 0:
            rates = [r + g for r, g in zip(rates, flux(states[layer - 1](), 1.0))]
        if layer < slab - 1:
            rates = [r + g for r, g in zip(rates, flux(states[layer + 1](), -1.0))]
        put(layer, rates)


def reader(ref, layer):
    return lambda: [ref[f, layer] for f in range(ref.shape[0])]


def readers(ref):
    return [reader(ref, layer) for layer in range(ref.shape[1])]


def edge_layers_kernel(state_ref, up_ref, down_ref):
    fields, slab = state_ref.shape[:2]
    for f in range(fields):
        up_ref[f] = state_ref[f, slab - 1]
        down_ref[f] = state_ref[f, 0]


def first_rate_kernel(
    state_ref,
    source_ref,
    table_ref,
    rate_ref,
    waves_ref,
    rate_up_ref,
    rate_down_ref,
    feed_up_ref,
    feed_down_ref,
    *,
    step,
):
    fields, slab, rows, cols = state_ref.shape
    last = slab - 1

    def put(layer, rates):
        for f in range(fields):
            rate_ref[f, layer] = rates[f]
            if layer == last:
                rate_up_ref[f] = rates[f]
            if layer == 0:
                rate_down_ref[f] = rates[f]
        for inner, edge, out_ref, sign in (
            (last - 1, last, feed_up_ref, 1.0),
            (1, 0, feed_down_ref, -1.0),
        ):
            if layer == inner:
                second = [state_ref[f, layer] + step * rates[f] for f in range(fields)]
                for f, value in enumerate(flux(second, sign)):
                    out_ref[f] = source_ref[f, edge] + value

    slab_rates(readers(state_ref), readers(source_ref), put)
    keep = table_ref.shape[0] // 4
    cells = state_ref[...].reshape(fields * slab * rows, cols)
    real, imag = by_field(along_x(cells, table_ref[...]), fields, keep)
    lanes = real.shape[1]
    waves_ref[:, :lanes] = real
    waves_ref[:, lanes:] = imag


def second_rate_kernel(
    state_ref,
    rate_ref,
    source_ref,
    below_ref,
    above_ref,
    next_ref,
    stage_ref,
    *,
    step,
):
    fields, slab = state_ref.shape[:2]
    for layer in range(slab):
        rates = [rate_ref[f, layer] for f in range(fields)]
        for edge, came_ref, sign in ((0, below_ref, 1.0), (slab - 1, above_ref, -1.0)):
            if layer == edge:
                given = flux([came_ref[f] for f in range(fields)], sign)
                rates = [rate + gift for rate, gift in zip(rates, given)]
        for f in range(fields):
            stage_ref[f, layer] = state_ref[f, layer] + step * rates[f]

    def put(layer, rates):
        for f in range(fields):
            next_ref[f, layer] = rates[f]

    slab_rates(readers(stage_ref), readers(source_ref), put)


def third_rate_kernel(
    state_ref,
    second_ref,
    rate_ref,
    source_ref,
    below_ref,
    above_ref,
    below_rate_ref,
    above_rate_ref,
    base_ref,
    edge_rate_ref,
    edge_sum_ref,
    inner_sum_ref,
    third_ref,
    fourth_ref,
    *,
    steps,
    weight,
):
    fields, slab, rows, cols = state_ref.shape
    last = slab - 1
    ids = range(fields)
    blank = [jnp.zeros((rows, cols), jnp.float32)] * fields
    for layer in range(1, last):
        for f in ids:
            third_ref[f, layer] = state_ref[f, layer] + steps[1] * rate_ref[f, layer]
    for side, edge, came_ref, came_rate_ref, sign in (
        (0, 0, below_ref, below_rate_ref, 1.0),
        (1, last, above_ref, above_rate_ref, -1.0),
    ):
        outward = flux([state_ref[f, edge] for f in ids], -sign)
        second = [came_ref[f] + steps[0] * (came_rate_ref[f] + outward[f]) for f in ids]
        for f, value in enumerate(flux(second, sign)):
            third_ref[f, edge] = state_ref[f, edge] + steps[1] * (rate_ref[f, edge] + value)
        outward = flux([second_ref[f, edge] for f in ids], -sign)
        rates = level_rate(second, outward)
        for f in ids:
            base_ref[side, f] = came_ref[f] + steps[1] * rates[f]

    def put(layer, rates):
        for f in ids:
            if 0 < layer < last:
                fourth_ref[f, layer - 1] = state_ref[f, layer] + steps[2] * rates[f]
            else:
                edge_rate_ref[0 if layer == 0 else 1, f] = rates[f]

    slab_rates(readers(third_ref), readers(source_ref), put)

    def so_far(f, layer):
        return (
            2.0 * third_ref[f, layer] + second_ref[f, layer] - state_ref[f, layer]
        ) * (1.0 / 3.0)

    def put_inner(index, rates):
        for f in ids:
            inner_sum_ref[f, index] = (
                so_far(f, index + 1) + fourth_ref[f, index] * (1.0 / 3.0) + weight * rates[f]
            )

    slab_rates(readers(fourth_ref), readers(source_ref)[1:last], put_inner)
    for side, edge, inner, sign in ((0, 0, 0, -1.0), (1, last, slab - 3, 1.0)):
        for f, value in enumerate(flux([fourth_ref[f, inner] for f in ids], sign)):
            edge_sum_ref[side, f] = so_far(f, edge) + weight * (source_ref[f, edge] + value)


def forward_kernel(
    state_ref,
    base_ref,
    edge_rate_ref,
    edge_sum_ref,
    inner_sum_ref,
    below_ref,
    above_ref,
    shifted_ref,
    table_ref,
    high_ref,
    low_ref,
    phase_ref,
    out_ref,
    inner_ref,
    outer_ref,
    *,
    steps,
    weight,
):
    fields, slab, rows, cols = state_ref.shape
    last = slab - 1
    ids = range(fields)
    blank = [jnp.zeros((rows, cols), jnp.float32)] * fields
    inward = {}
    for side, edge, came_ref, sign in ((0, 0, below_ref, 1.0), (1, last, above_ref, -1.0)):
        third = [base_ref[side, f] + steps[1] * came_ref[f] for f in ids]
        given = flux(third, sign)
        fourth = [
            state_ref[f, edge] + steps[2] * (edge_rate_ref[side, f] + given[f]) for f in ids
        ]
        rates = level_rate(fourth, blank)
        for f in ids:
            inner_ref[f, edge] = (
                edge_sum_ref[side, f] + fourth[f] * (1.0 / 3.0) + weight * rates[f]
            )
        for f, value in enumerate(flux(fourth, -sign)):
            outer_ref[side, f] = weight * value
        inner = 1 if side == 0 else last - 1
        for f, value in enumerate(flux(fourth, sign)):
            earlier = inner_ref if inner in inward else inner_sum_ref
            shift = 0 if inner in inward else 1
            inner_ref[f, inner] = earlier[f, inner - shift] + weight * value
        inward[inner] = True
    for layer in range(1, last):
        if layer not in inward:
            for f in ids:
                inner_ref[f, layer] = inner_sum_ref[f, layer - 1]

    width = out_ref.shape[0]
    keep = table_ref.shape[0] // 4
    half = out_ref.shape[2] // 2
    place = lax.axis_index("space")
    table = table_ref[...]
    real, imag = by_field(
        along_x(inner_ref[...].reshape(fields * slab * rows, cols), table), fields, keep
    )
    outer_cells = jnp.concatenate(
        [outer_ref[side, f] for f in range(fields) for side in range(2)]
    )
    outer_real, outer_imag = by_field(along_x(outer_cells, table), fields, keep)
    shifted = shifted_ref[...]
    lanes = real.shape[1]
    left = jnp.concatenate(
        [real - shifted[:, :lanes], imag - shifted[:, lanes:], outer_real, outer_imag], axis=1
    )
    waves = three_pass(left, high_ref[...], low_ref[...])
    for group in range(width):
        block = waves[:, group * 2 * half : (group + 1) * 2 * half]
        turned = (
            block * phase_ref[place, 0, group, :][None, :]
            + pltpu.roll(block, half, 1) * phase_ref[place, 1, group, :][None, :]
        )
        out_ref[step_between(place, group, width)] = turned


def coarse_kernel(jump_ref, symbol_ref, share_ref, out_ref, kept_ref, *, plane):
    slices, lines, lanes = jump_ref.shape
    keep = share_ref.shape[0]
    fields = lines // keep
    place = lax.axis_index("space")
    moment = lax.axis_index("tm")
    real = symbol_ref[place, 0]
    imag = symbol_ref[place, 1]
    share = share_ref[...]
    blank = jnp.zeros((keep, lanes), jnp.float32)
    current = [(blank, blank)] * fields
    sizes = []
    kept_ref[0] = jnp.zeros((lines, lanes), jnp.float32)
    for moment_id in range(slices):
        total = blank
        for value, _ in current:
            total = total + value * value
        sizes.append(jnp.sum(total * share, axis=0, keepdims=True))
        if moment_id == slices - 1:
            break
        for f in range(fields):
            jump = jump_ref[moment_id, f * keep : (f + 1) * keep, :]
            value = jump + current[f][0]
            swapped = pltpu.roll(jump, lanes // 2, 1) + current[f][1]
            current[f] = (value * real + swapped * imag, swapped * real - value * imag)
            kept_ref[moment_id + 1, f * keep : (f + 1) * keep, :] = current[f][0]
    sums = jnp.sum(jnp.concatenate(sizes), axis=1, keepdims=True)
    lane = lax.broadcasted_iota(jnp.int32, (lines, lanes), 1)
    message = kept_ref[moment]
    for chunk in range(-(-slices // lines)):
        column = sums[chunk * lines : (chunk + 1) * lines]
        spare = lines - column.shape[0]
        if spare > 0:
            column = jnp.concatenate([column, jnp.zeros((spare, 1), jnp.float32)])
        message = jnp.where(lane == chunk * plane + plane // 2, column, message)
    out_ref[...] = message


def uncorrected_kernel(fine_ref, below_ref, above_ref, ends_ref, held_ref, sems):
    fields, slab = fine_ref.shape[:2]

    @pl.when(lax.axis_index("tm") == 0)
    def _():
        copies = []
        for f in range(fields):
            for layer in range(slab):
                value = fine_ref[f, layer]
                if layer == 0:
                    value = value + below_ref[f]
                if layer == slab - 1:
                    value = value + above_ref[f]
                held_ref[f, layer] = value
            copies.append(pltpu.make_async_copy(held_ref.at[f], ends_ref.at[f], sems.at[f]))
            copies[-1].start()
        for copy in copies:
            copy.wait()


def inverse_kernel(*refs, width, slices, plane, scales):
    block_refs = refs[:width]
    (
        fine_ref,
        below_ref,
        above_ref,
        high_ref,
        low_ref,
        table_ref,
        phase_ref,
        _,
        ends_ref,
        slice_ref,
        total_ref,
        order_ref,
        held_ref,
        own_norm_ref,
        whole_norm_ref,
        sems,
        norm_sems,
    ) = refs[width:]
    fields, slab, rows, cols = fine_ref.shape
    place = lax.axis_index("space")
    moment = lax.axis_index("tm")
    lines, lanes = order_ref.shape[1:]
    keep = lines // fields

    total = block_refs[0][...]
    for step in range(1, width):
        total = total + block_refs[step][...]
    line = lax.broadcasted_iota(jnp.int32, (lines, 1), 0)
    lane = lax.broadcasted_iota(jnp.int32, (lines, lanes), 1)
    own, whole = jnp.zeros((1, 1), jnp.float32), jnp.zeros((1, 1), jnp.float32)
    for chunk in range(-(-slices // lines)):
        spot = lane == chunk * plane + plane // 2
        column = jnp.sum(jnp.where(spot, total, 0.0), axis=1, keepdims=True)
        here = jnp.where(line + chunk * lines == moment, column, 0.0)
        own = own + jnp.sum(here, axis=0, keepdims=True)
        whole = whole + jnp.sum(column, axis=0, keepdims=True)
    own_norm_ref[...] = jnp.sqrt(own * scales[0] + epsilon)
    whole_norm_ref[...] = jnp.sqrt(whole * scales[1] + epsilon)
    norms = [
        pltpu.make_async_copy(own_norm_ref, slice_ref, norm_sems.at[0]),
        pltpu.make_async_copy(whole_norm_ref, total_ref, norm_sems.at[1]),
    ]
    for copy in norms:
        copy.start()

    @pl.when(moment != 0)
    def _():
        for step in range(width):
            group = source_of(place, step, width)
            block = block_refs[step][...]
            order_ref[group] = (
                block * phase_ref[place, 0, group, :][None, :]
                - pltpu.roll(block, lanes // 2, 1) * phase_ref[place, 1, group, :][None, :]
            )
        left = jnp.concatenate([order_ref[group] for group in range(width)], axis=1)
        waves = three_pass(left, high_ref[...], low_ref[...])
        count = slab * rows
        copies = []
        for f in range(fields):
            own_waves = waves[f * keep : (f + 1) * keep]
            high, low = split(jnp.concatenate([own_waves[:, :count], own_waves[:, count:]]))
            change = lax.dot_general(
                jnp.concatenate([high, low, high]),
                table_ref[...],
                (((0,), (0,)), ((), ())),
                preferred_element_type=jnp.float32,
            ).reshape(slab, rows, cols)
            for layer in range(slab):
                value = fine_ref[f, layer] + change[layer]
                if layer == 0:
                    value = value + below_ref[f]
                if layer == slab - 1:
                    value = value + above_ref[f]
                held_ref[f, layer] = value
            copies.append(pltpu.make_async_copy(held_ref.at[f], ends_ref.at[f], sems.at[f]))
            copies[-1].start()
        for copy in copies:
            copy.wait()

    for copy in norms:
        copy.wait()


def halo(up, down):
    count = lax.axis_size("space")
    ups = [(i, (i + 1) % count) for i in range(count)]
    downs = [((i + 1) % count, i) for i in range(count)]
    return lax.ppermute(up, "space", ups), lax.ppermute(down, "space", downs)


def shards(starts, source):
    state_now = starts[0]
    fields, slab, rows, cols = state_now.shape
    width = lax.axis_size("space")
    slices = lax.axis_size("tm")
    depth = slab * width
    keep_y, keep_x = rows // 8, cols // 16
    lines, lanes = fields * keep_x, 2 * slab * 2 * keep_y
    tables = make_tables(slab, width, rows, cols)
    real = jnp.float32

    layer_shape = jax.ShapeDtypeStruct((fields, rows, cols), real)
    edge_shape = jax.ShapeDtypeStruct((2, fields, rows, cols), real)
    slab_shape = jax.ShapeDtypeStruct((fields, slab, rows, cols), real)
    inner_shape = jax.ShapeDtypeStruct((fields, slab - 2, rows, cols), real)
    steps = (0.5 * time_step, 0.5 * time_step, time_step)
    weight = time_step / 6.0

    up, down = local_call(edge_layers_kernel, (layer_shape, layer_shape), [state_now])
    below, above = halo(up, down)
    rates, start_waves, *given = local_call(
        functools.partial(first_rate_kernel, step=steps[0]),
        (
            slab_shape,
            jax.ShapeDtypeStruct((lines, 2 * slab * rows), real),
            *(layer_shape,) * 4,
        ),
        [state_now, source, tables["xforward"]],
    )
    below_rate, above_rate = halo(given[0], given[1])
    below_feed, above_feed = halo(given[2], given[3])
    next_waves = lax.ppermute(start_waves, "tm", [(i + 1, i) for i in range(slices - 1)])
    rates, second = local_call(
        functools.partial(second_rate_kernel, step=steps[0]),
        (slab_shape, slab_shape),
        [state_now, rates, source, below, above],
    )
    base, edge_rate, edge_sum, inner_sum = local_call(
        functools.partial(third_rate_kernel, steps=steps, weight=weight),
        (edge_shape, edge_shape, edge_shape, inner_shape),
        [state_now, second, rates, source, below, above, below_rate, above_rate],
        [
            pltpu.VMEM((fields, slab, rows, cols), real),
            pltpu.VMEM((fields, slab - 2, rows, cols), real),
        ],
    )
    waves, fine_inner, fine_outer = local_call(
        functools.partial(forward_kernel, steps=steps, weight=weight),
        (jax.ShapeDtypeStruct((width, lines, lanes), real), slab_shape, edge_shape),
        [
            state_now,
            base,
            edge_rate,
            edge_sum,
            inner_sum,
            below_feed,
            above_feed,
            next_waves,
            tables["xforward"],
            *tables["yzforward"],
            tables["phase"],
        ],
    )
    jump = waves[0]
    for step in range(1, width):
        part = lax.ppermute(
            waves[step], "space", [(i, target_of(i, step, width)) for i in range(width)]
        )
        jump = jump + part

    below, above = halo(fine_outer[1], fine_outer[0])

    jumps = lax.all_to_all(jnp.broadcast_to(jump, (slices, lines, lanes)), "tm", 0, 0, tiled=True)

    message = local_call(
        functools.partial(coarse_kernel, plane=2 * keep_y),
        jax.ShapeDtypeStruct((lines, lanes), real),
        [jumps, tables["symbol"], tables["share"]],
        [pltpu.VMEM((slices, lines, lanes), real)],
    )
    blocks = [message]
    for step in range(1, width):
        block = lax.ppermute(
            message, "space", [(i, target_of(i, step, width)) for i in range(width)]
        )
        blocks.append(block)
    whole_slab = pltpu.VMEM((fields, slab, rows, cols), real)
    ends = local_call(
        uncorrected_kernel,
        jax.ShapeDtypeStruct((fields, slab, rows, cols), real),
        [fine_inner, below, above],
        [whole_slab, pltpu.SemaphoreType.DMA((fields,))],
        out_specs=off_chip,
    )
    cells = fields * depth * rows * cols
    ends, slice_norm, total_norm = local_call(
        functools.partial(
            inverse_kernel, width=width, slices=slices, plane=2 * keep_y, scales=(1.0 / cells, 1.0 / (cells * slices))
        ),
        (
            jax.ShapeDtypeStruct((fields, slab, rows, cols), real),
            jax.ShapeDtypeStruct((1, 1), real),
            jax.ShapeDtypeStruct((1, 1), real),
        ),
        [
            *blocks,
            fine_inner,
            below,
            above,
            *tables["yzinverse"],
            tables["xinverse"],
            tables["phase"],
            ends,
        ],
        [
            pltpu.VMEM((width, lines, lanes), real),
            whole_slab,
            pltpu.VMEM((1, 1), real),
            pltpu.VMEM((1, 1), real),
            pltpu.SemaphoreType.DMA((fields,)),
            pltpu.SemaphoreType.DMA((2,)),
        ],
        places={width + 7: off_chip},
        out_specs=(off_chip, off_chip, off_chip),
        aliases={width + 7: 0},
    )
    return ends[None], slice_norm[0], total_norm[0]


def solution(mesh):
    in_specs = (P("tm", None, "space", None, None), P(None, "space", None, None))
    out_specs = (P("tm", None, "space", None, None), P("tm"), P())
    return jax.shard_map(shards, mesh=mesh, in_specs=in_specs, out_specs=out_specs, check_vma=False)
```
